32 devices in a mesh: dp: 1 (over z), tp: 32 (over y, x, core).
Axes of the slice: x: 4, y: 4, z: 1, core: 2. Of those that a mesh axis runs over, the one named last changes fastest.
The devices are a block of a 4x4x8 slice.
Arguments:
- resid_in: bfloat16 [512, 2048], P('dp')
- cand_ids: int32 [512, 256], P('dp')
- ln_mlp: bfloat16 [2048], replicated
- wi_gate: bfloat16 [2048, 5120], P(None, 'tp')
- wi_lin: bfloat16 [2048, 5120], P(None, 'tp')
- w_out: bfloat16 [5120, 2048], P('tp')
- ln_final: bfloat16 [2048], replicated
- w_lm: bfloat16 [2048, 256384], P(None, 'tp')
Outputs:
- output 1: float32 [512, 256], P('dp')
- output 2: float32 [512], P('dp')
All inputs are finite; a program needn't handle non-finite values.
Results may differ from the reference program's by a relative error of at most 0.00164064.
Values sent between devices are 32-bit elements.
A program may use at most 768 MiB of HBM per device.

```python
import math
import jax
import jax.numpy as jnp
from jax import lax

BATCH = 512
CANDS = 256
D_MODEL = 2048
D_FF = 5120
VOCAB = 256384

EPS = 1e-6
ROW_BLOCK = min(8, BATCH)
LOW_IDS = VOCAB // 16
LOGIT_STD = math.sqrt(math.log(VOCAB))


def rms_norm(values_in, scale_vec):
    wide = values_in.astype(jnp.float32)
    mean_sq = jnp.mean(wide * wide, axis=-1, keepdims=True)
    return (wide * lax.rsqrt(mean_sq + EPS) * scale_vec.astype(jnp.float32)).astype(jnp.bfloat16)


def draw_cands(cand_key):
    key_pick, key_low, key_any = jax.random.split(cand_key, 3)
    pick_low = jax.random.randint(key_pick, (BATCH, CANDS), 0, 2) == 0
    low_ids = jax.random.randint(key_low, (BATCH, CANDS), 0, LOW_IDS)
    any_ids = jax.random.randint(key_any, (BATCH, CANDS), 0, VOCAB)
    cand_ids = jnp.where(pick_low, low_ids, any_ids)
    cand_ids = cand_ids.at[0, 0].set(0).at[0, CANDS - 1].set(VOCAB - 1)
    return cand_ids.astype(jnp.int32)


def draw_lm(lm_key):
    def one_block(block_idx):
        block = jax.random.normal(jax.random.fold_in(lm_key, block_idx), (128, VOCAB), jnp.float32)
        return (block * (LOGIT_STD / math.sqrt(D_MODEL))).astype(jnp.bfloat16)
    return lax.map(one_block, jnp.arange(D_MODEL // 128)).reshape(D_MODEL, VOCAB)


def setup_inputs(seed: int = 0, part: int = 0) -> dict:
    base_key = jax.random.key(seed)
    key_x, key_cand = jax.random.split(jax.random.fold_in(base_key, part), 2)
    shared = jax.random.split(base_key, 6)
    resid_in = jax.random.normal(key_x, (BATCH, D_MODEL), jnp.float32).astype(jnp.bfloat16)
    ln_mlp = (1.0 + 0.3 * jax.random.normal(shared[0], (D_MODEL,), jnp.float32)).astype(jnp.bfloat16)
    wi_gate = (jax.random.normal(shared[1], (D_MODEL, D_FF), jnp.float32) / math.sqrt(D_MODEL)).astype(jnp.bfloat16)
    wi_lin = (jax.random.normal(shared[2], (D_MODEL, D_FF), jnp.float32) / math.sqrt(D_MODEL)).astype(jnp.bfloat16)
    w_out = (jax.random.normal(shared[3], (D_FF, D_MODEL), jnp.float32) * (1.5 / math.sqrt(D_FF))).astype(jnp.bfloat16)
    ln_final = (1.0 + 0.3 * jax.random.normal(shared[4], (D_MODEL,), jnp.float32)).astype(jnp.bfloat16)
    return {"resid_in": resid_in, "cand_ids": draw_cands(key_cand), "ln_mlp": ln_mlp, "wi_gate": wi_gate, "wi_lin": wi_lin, "w_out": w_out, "ln_final": ln_final, "w_lm": draw_lm(shared[5])}


def reference(resid_in, cand_ids, ln_mlp, wi_gate, wi_lin, w_out, ln_final, w_lm):
    normed = rms_norm(resid_in, ln_mlp)
    act_gate = jnp.dot(normed, wi_gate, preferred_element_type=jnp.float32)
    act_lin = jnp.dot(normed, wi_lin, preferred_element_type=jnp.float32)
    hidden = (jax.nn.gelu(act_gate, approximate=True) * act_lin).astype(jnp.bfloat16)
    mlp_out = jnp.dot(hidden, w_out, preferred_element_type=jnp.float32)
    resid_out = (resid_in.astype(jnp.float32) + mlp_out).astype(jnp.bfloat16)
    final_z = rms_norm(resid_out, ln_final)

    def row_block(block_args):
        z_rows, id_rows = block_args
        logits = jnp.dot(z_rows, w_lm, preferred_element_type=jnp.float32)
        row_max = jnp.max(logits, axis=-1)
        norm_rows = row_max + jnp.log(jnp.sum(jnp.exp(logits - row_max[:, None]), axis=-1))
        picked = jnp.take_along_axis(logits, id_rows, axis=1)
        return picked - norm_rows[:, None], norm_rows

    num_blocks = BATCH // ROW_BLOCK
    log_probs, log_norm = lax.map(row_block, (final_z.reshape(num_blocks, ROW_BLOCK, D_MODEL), cand_ids.reshape(num_blocks, ROW_BLOCK, CANDS)))
    return log_probs.reshape(BATCH, CANDS), log_norm.reshape(BATCH)
```

```python
import functools
import math

import jax
import jax.numpy as jnp
from jax import lax
from jax.experimental import pallas as pl
from jax.experimental.pallas import tpu as pltpu
from jax.sharding import PartitionSpec as P

EPS = 1e-6
LANES = 128
CORES = 2
MESH = pl.DeviceIdType.MESH
NEG = float("-inf")

NORTH = False
ROWS_LM = 128
TILE = 256


def rms_rows(wide, scale):
    mean_sq = jnp.mean(wide * wide, axis=-1, keepdims=True)
    return (wide * lax.rsqrt(mean_sq + EPS) * scale).astype(jnp.bfloat16)


def log_add(parts):
    top = functools.reduce(jnp.maximum, parts)
    total = functools.reduce(jnp.add, [jnp.exp(p - top) for p in parts])
    return top + jnp.log(total)


class Link:
    def __init__(self, src, dst, send, recv, to):
        self.args = dict(
            src_ref=src, dst_ref=dst, send_sem=send, recv_sem=recv,
            device_id={"tp": to}, device_id_type=MESH,
        )

    def make(self):
        return pltpu.make_async_remote_copy(**self.args)

    def start(self):
        self.make().start()

    def sent(self):
        self.make().wait_send()

    def came(self):
        self.make().wait_recv()


def fused(cfg, x_hbm, ids_hbm, lnm_ref, wg_hbm, wl_hbm, wo_hbm, lnf_ref, w_hbm,
          lp_hbm, ln_hbm,
          x_v, ids_v, wg_v, wl_v, wo_v, w_v, z_v, lg_v, st_v, lse_v, lnrow_v, ob_v,
          bufs, tails, send_sems, recv_sems, loc_sems):
    q, chunks, lm_chunks = cfg["q"], cfg["chunks"], cfg["lm"]
    me = lax.axis_index("tp")
    core = lax.rem(me, CORES)
    x = lax.rem(me // CORES, q)
    y = me // (CORES * q)
    sibling = me + 1 - 2 * core
    vocab = w_v.shape[1]
    ndev_side = q

    if NORTH:
        slots = [0, 1]
        half_of = [0, 1]
        speak = 1
    else:
        slots = [0]
        half_of = [core]
        speak = core

    def coords(s):
        if NORTH:
            return (x, y) if s == 0 else (y, x)
        a = jnp.where(core == 0, x, y)
        b = jnp.where(core == 0, y, x)
        return a, b

    def device(s, a, b):
        if NORTH:
            col, row = (a, b) if s == 0 else (b, a)
            return (row * q + col) * CORES + 1
        col = jnp.where(core == 0, a, b)
        row = jnp.where(core == 0, b, a)
        return (row * q + col) * CORES + core

    def step(v, d):
        return lax.rem(v + d + q, q)

    counter = [0]
    started = {"all": [], "talk": [], "quiet": []}

    def link(src, dst, to, who="talk"):
        i = counter[0]
        counter[0] += 1
        made = Link(src, dst, send_sems.at[i], recv_sems.at[i], to)
        started[who].append(made)
        return made

    def talkers(fn):
        if NORTH:
            pl.when(core == 1)(fn)
        else:
            fn()

    def quiet(fn):
        if NORTH:
            pl.when(core == 0)(fn)

    loads = {}
    loc_count = [0]

    def load(name, src, dst):
        i = loc_count[0]
        loc_count[0] += 1
        cp = pltpu.make_async_copy(src, dst, loc_sems.at[i])
        loads[name] = cp
        cp.start()

    off0, rows0 = chunks[0]
    load("x0", x_hbm.at[pl.ds(off0, rows0), :], x_v.at[pl.ds(off0, rows0), :])
    load("wg", wg_hbm, wg_v)
    load("wl", wl_hbm, wl_v)
    load("wo", wo_hbm, wo_v)
    for k, (off, rows) in enumerate(chunks[1:], 1):
        load(f"x{k}", x_hbm.at[pl.ds(off, rows), :], x_v.at[pl.ds(off, rows), :])
    load("ids", ids_hbm, ids_v)
    parts = cfg["w_parts"]
    depth = w_v.shape[0] // parts
    for i in range(parts):
        load(f"w{i}", w_hbm.at[pl.ds(i * depth, depth), :], w_v.at[pl.ds(i * depth, depth), :])

    barrier = pltpu.get_barrier_semaphore()

    def greet(to):
        pl.semaphore_signal(barrier, inc=1, device_id={"tp": to}, device_id_type=MESH)

    greet(sibling)

    def greet_far():
        a, b = coords(0)
        for d in range(1, q):
            greet(device(0, step(a, d), b))
            greet(device(0, a, step(b, d)))

    talkers(greet_far)

    def meet():
        if NORTH:
            pl.when(core == 1)(lambda: pl.semaphore_wait(barrier, 1 + 2 * (q - 1)))
            pl.when(core == 0)(lambda: pl.semaphore_wait(barrier, 1))
        else:
            pl.semaphore_wait(barrier, 1 + 2 * (q - 1))

    scale_mlp = lnm_ref[...].astype(jnp.float32)
    scale_fin = lnf_ref[...].astype(jnp.float32)

    plans = []
    for k, (off, rows) in enumerate(chunks):
        r2 = rows // 2
        hr = r2 // 2
        px, dr, rl, dc, cb, bs, pr, xb = bufs[k]
        plan = {"slots": []}
        if NORTH:
            plan["pair"] = [link(px.at[h], dr.at[h], sibling, "quiet") for h in (0, 1)]
        else:
            plan["pair"] = [link(px.at[1 - core], dr.at[0], sibling)]
        for s in slots:
            a, b = coords(s)
            h = half_of[s]
            up, down, far = step(a, 1), step(a, -1), step(a, 2)
            to_up, to_down = device(s, up, b), device(s, down, b)
            lo, hi = pl.ds(0, hr), pl.ds(hr, hr)

            def grp(v):
                return pl.ds(v * q, q)

            e = {}
            e["relay"] = [
                link(dr.at[s, grp(far), lo, :], rl.at[s, 0], to_up),
                link(dr.at[s, grp(far), hi, :], rl.at[s, 1], to_down),
            ]
            e["direct"] = [
                link(dr.at[s, grp(down), lo, :], dc.at[s, 0], to_down),
                link(dr.at[s, grp(up), hi, :], dc.at[s, 1], to_up),
            ]
            e["comb"] = [
                link(rl.at[s, 0], cb.at[s, 0], to_up),
                link(rl.at[s, 1], cb.at[s, 1], to_down),
            ]
            e["second"] = [
                link(bs.at[s, step(b, d)], pr.at[s, d - 1], device(s, a, step(b, d)))
                for d in range(1, q)
            ]
            own = xb.at[h, a * q + b]
            e["spread2"] = [link(own, own, device(s, a, step(b, d))) for d in range(1, q)]
            mine_lo = xb.at[h, grp(a), lo, :]
            mine_hi = xb.at[h, grp(a), hi, :]
            e["up"] = [link(mine_lo, mine_lo, to_up), link(mine_hi, mine_hi, to_up)]
            e["down"] = [link(mine_lo, mine_lo, to_down), link(mine_hi, mine_hi, to_down)]
            fwd_lo = xb.at[h, grp(down), lo, :]
            fwd_hi = xb.at[h, grp(up), hi, :]
            e["fwd"] = [link(fwd_lo, fwd_lo, to_up), link(fwd_hi, fwd_hi, to_down)]
            e["pass"] = [
                link(xb.at[h, grp(step(a, d))], xb.at[h, grp(step(a, d))], sibling)
                for d in range(q)
            ]
            plan["slots"].append(e)
        plans.append(plan)

    def mlp(k):
        off, rows = chunks[k]
        px = bufs[k][0]
        r2 = rows // 2
        loads[f"x{k}"].wait()
        wide = x_v[pl.ds(off, rows), :].astype(jnp.float32)
        normed = rms_rows(wide, scale_mlp)
        if k == 0:
            loads["wg"].wait()
            loads["wl"].wait()
        gate = jnp.dot(normed, wg_v[...], preferred_element_type=jnp.float32)
        lin = jnp.dot(normed, wl_v[...], preferred_element_type=jnp.float32)
        hidden = (jax.nn.gelu(gate, approximate=True) * lin).astype(jnp.bfloat16)
        if k == 0:
            loads["wo"].wait()
        part = jnp.dot(hidden, wo_v[...], preferred_element_type=jnp.float32)
        for h in range(2):
            for j in range(q * q):
                px[h, j] = part[h * r2:(h + 1) * r2, j * LANES:(j + 1) * LANES]

    def pair_send(k):
        def go():
            for l in plans[k]["pair"]:
                l.start()
        if NORTH:
            quiet(go)
        else:
            go()

    def first_send(k):
        px, dr = bufs[k][0], bufs[k][1]

        def go():
            for l in plans[k]["pair"]:
                l.came()
            for s in slots:
                a, _ = coords(s)
                h = half_of[s]
                e = plans[k]["slots"][s]
                for d in (2, 1, 3, 0):
                    g = pl.ds(step(a, d) * q, q)
                    dr[s, g] = dr[s, g] + px[h, g]
                    if d == 2:
                        for l in e["relay"]:
                            l.start()
                    if d == 3:
                        for l in e["direct"]:
                            l.start()
        talkers(go)

    def first_relay(k):
        _, dr, rl = bufs[k][:3]
        hr = chunks[k][1] // 4

        def go():
            for s in slots:
                a, _ = coords(s)
                e = plans[k]["slots"][s]
                for i, d in ((0, 1), (1, -1)):
                    e["relay"][i].came()
                    g = pl.ds(step(a, d) * q, q)
                    rl[s, i] = rl[s, i] + dr[s, g, i * hr:(i + 1) * hr, :]
                    e["comb"][i].start()
        talkers(go)

    def second_send(k):
        _, dr, _, dc, cb, bs = bufs[k][:6]
        hr = chunks[k][1] // 4

        def go():
            for s in slots:
                a, _ = coords(s)
                e = plans[k]["slots"][s]
                g = pl.ds(a * q, q)
                for i in range(2):
                    e["direct"][i].came()
                    e["comb"][i].came()
                    part = slice(i * hr, (i + 1) * hr)
                    bs[s, :, part, :] = dr[s, g, part, :] + dc[s, i] + cb[s, i]
                for l in e["second"]:
                    l.start()
        talkers(go)

    def own_block(k):
        off, rows = chunks[k]
        r2 = rows // 2
        bs, pr, xb = bufs[k][5:]

        def go():
            for s in slots:
                a, b = coords(s)
                h = half_of[s]
                e = plans[k]["slots"][s]
                for l in e["second"]:
                    l.came()
                total = bs[s, b]
                for d in range(q - 1):
                    total = total + pr[s, d]
                col = pl.ds(pl.multiple_of((a * q + b) * LANES, LANES), LANES)
                row = pl.ds(pl.multiple_of(off + h * r2, 16), r2)
                resid = x_v[row, col].astype(jnp.float32)
                xb[h, a * q + b] = (resid + total).astype(jnp.bfloat16).astype(jnp.float32)
                for l in e["spread2"]:
                    l.start()
        talkers(go)

    def spread_first(k):
        def go():
            for s in slots:
                e = plans[k]["slots"][s]
                for l in e["spread2"]:
                    l.came()
                e["up"][0].start()
                e["down"][1].start()
                e["up"][1].start()
                e["down"][0].start()
                e["pass"][0].start()
        talkers(go)

    def spread_forward(k):
        def go():
            for s in slots:
                e = plans[k]["slots"][s]
                e["up"][0].came()
                e["fwd"][0].start()
                e["down"][1].came()
                e["fwd"][1].start()
        talkers(go)

    def spread_last(k):
        def go():
            for s in slots:
                e = plans[k]["slots"][s]
                e["up"][1].came()
                e["pass"][q - 1].start()
                e["down"][0].came()
                e["pass"][1].start()
                for l in e["fwd"]:
                    l.came()
                e["pass"][2].start()
        talkers(go)

    def arrive(k):
        def go():
            for s in slots:
                for l in plans[k]["slots"][s]["pass"]:
                    l.came()
        if NORTH:
            quiet(go)
        else:
            go()

    def normalize(l):
        first = lm_chunks[l]
        base = chunks[first[0]][0]
        for k in first:
            off, rows = chunks[k]
            r2 = rows // 2
            xb = bufs[k][7]
            for h in range(2):
                sq = None
                for j in range(q * q):
                    v = xb[h, j]
                    sq = v * v if sq is None else sq + v * v
                mean_sq = jnp.sum(sq, axis=-1, keepdims=True) * (1.0 / (q * q * LANES))
                inv = jnp.broadcast_to(lax.rsqrt(mean_sq + EPS), (r2, LANES))
                for j in range(q * q):
                    cols = slice(j * LANES, (j + 1) * LANES)
                    z_v[off - base + h * r2:off - base + (h + 1) * r2, cols] = (
                        xb[h, j] * inv * scale_fin[:, cols]
                    ).astype(jnp.bfloat16)

    n_tiles = -(-vocab // TILE)

    def lm(l, t0, t1):
        rows = ROWS_LM
        base = chunks[lm_chunks[l][0]][0]
        loc = [ids_v[base:base + rows, c * LANES:(c + 1) * LANES] - me * vocab for c in range(2)]
        chunk = [jnp.where((v >= 0) & (v < vocab), lax.shift_right_arithmetic(v, 7), -1) for v in loc]
        lane = [v & (LANES - 1) for v in loc]
        if t0 == 0:
            top = total = None
            pick = [jnp.zeros((rows, LANES), jnp.float32) for _ in range(2)]
        else:
            top, total, pick = st_v[0], st_v[1], [st_v[2], st_v[3]]
        z = z_v[...]
        for t in range(t0, t1):
            a = t * TILE
            wd = min(TILE, vocab - a)
            slot = t % 2
            lg_v[slot, :, :wd] = jnp.dot(z, w_v[:, a:a + wd], preferred_element_type=jnp.float32)
            nv = -(-wd // LANES)
            xs = [lg_v[slot, :, j * LANES:(j + 1) * LANES] for j in range(nv)]
            if wd % LANES:
                pos = lax.broadcasted_iota(jnp.int32, (rows, LANES), 1)
                xs[-1] = jnp.where(pos < wd % LANES, xs[-1], NEG)
            peak = functools.reduce(jnp.maximum, xs)
            new = peak if top is None else jnp.maximum(top, peak)
            acc = None if total is None else total * jnp.exp(top - new)
            for v in xs:
                ev = jnp.exp(v - new)
                acc = ev if acc is None else acc + ev
            top, total = new, acc
            for c in range(2):
                for j in range(nv):
                    got = jnp.take_along_axis(xs[j], lane[c], axis=1, mode="promise_in_bounds")
                    pick[c] = jnp.where(chunk[c] == a // LANES + j, got, pick[c])
        if t1 < n_tiles:
            st_v[0], st_v[1], st_v[2], st_v[3] = top, total, pick[0], pick[1]
            return
        peak = jnp.max(top, axis=-1, keepdims=True)
        mass = jnp.sum(total * jnp.exp(top - peak), axis=-1, keepdims=True)
        part = jnp.broadcast_to(peak + jnp.log(mass), (rows, LANES))
        flat = part.T[0:8, :]
        tp = tails[l][0]
        r2 = rows // 2
        for h in range(2):
            for c in range(2):
                cols = slice(c * LANES, (c + 1) * LANES)
                tp[h, 0:r2, cols] = pick[c][h * r2:(h + 1) * r2, :]
                tp[h, r2:r2 + 8, cols] = flat

    r2 = ROWS_LM // 2
    tplans = []
    for l in range(len(lm_chunks)):
        tp, t1r, t2r, t3r, tc = tails[l]
        plan = {"slots": []}
        if NORTH:
            plan["pair"] = [link(tp.at[h], t1r.at[h], sibling, "quiet") for h in (0, 1)]
        else:
            plan["pair"] = [link(tp.at[1 - core], t1r.at[0], sibling)]
        for s in slots:
            a, b = coords(s)
            h = half_of[s]
            plan["slots"].append({
                "one": [link(t2r.at[s, a], t2r.at[s, a], device(s, step(a, d), b)) for d in range(1, q)],
                "two": [link(t3r.at[s, b], t3r.at[s, b], device(s, a, step(b, d))) for d in range(1, q)],
                "back": [link(tc.at[h], tc.at[h], sibling)],
            })
        tplans.append(plan)

    def join(refs, out):
        total = functools.reduce(jnp.add, [r[0:r2, :] for r in refs])
        out[0:r2, :] = total
        out[r2:r2 + 8, :] = log_add([r[r2:r2 + 8, :] for r in refs])

    def tail_pair(l):
        def go():
            for k in tplans[l]["pair"]:
                k.start()
        if NORTH:
            quiet(go)
        else:
            go()

    def tail_one(l):
        tp, t1r, t2r = tails[l][:3]

        def go():
            for k in tplans[l]["pair"]:
                k.came()
            for s in slots:
                join([tp.at[half_of[s]], t1r.at[s]], t2r.at[s, coords(s)[0]])
                for k in tplans[l]["slots"][s]["one"]:
                    k.start()
        talkers(go)

    def tail_two(l):
        t2r, t3r = tails[l][2:4]

        def go():
            for s in slots:
                for k in tplans[l]["slots"][s]["one"]:
                    k.came()
                join([t2r.at[s, d] for d in range(q)], t3r.at[s, coords(s)[1]])
                for k in tplans[l]["slots"][s]["two"]:
                    k.start()
        talkers(go)

    def tail_three(l):
        t3r, tc = tails[l][3:5]

        def go():
            for s in slots:
                for k in tplans[l]["slots"][s]["two"]:
                    k.came()
                join([t3r.at[s, d] for d in range(q)], tc.at[half_of[s]])
                for k in tplans[l]["slots"][s]["back"]:
                    k.start()
        talkers(go)

    outs = []

    def tail_done(l):
        tc = tails[l][4]

        def go():
            for s in slots:
                for k in tplans[l]["slots"][s]["back"]:
                    k.came()
        if NORTH:
            quiet(go)
        else:
            go()
        base = chunks[lm_chunks[l][0]][0]
        row = tc[0, r2:r2 + 1, 0:LANES]
        lnrow_v[l:l + 1, :] = row
        lse = jnp.broadcast_to(row, (LANES, LANES)).T
        for h in range(2):
            for c in range(2):
                cols = slice(c * LANES, (c + 1) * LANES)
                ob_v[base + h * r2:base + (h + 1) * r2, cols] = (
                    tc[h, 0:r2, cols] - lse[h * r2:(h + 1) * r2, :]
                )
        i = loc_count[0]
        loc_count[0] += 1
        cp = pltpu.make_async_copy(
            ob_v.at[base:base + ROWS_LM, :], lp_hbm.at[base:base + ROWS_LM, :], loc_sems.at[i])
        cp.start()
        outs.append(cp)

    stages = [mlp, pair_send, first_send, first_relay, second_send, own_block,
              spread_first, spread_forward, spread_last]
    names = {f.__name__: f for f in stages}
    names.update({f.__name__: f for f in (arrive, normalize, tail_pair, tail_one, tail_two, tail_three, tail_done)})
    for item in cfg["order"]:
        what, arg = item[0], item[1:]
        if what == "meet":
            meet()
        elif what == "weights":
            for i in range(parts):
                loads[f"w{i}"].wait()
        elif what == "ids":
            loads["ids"].wait()
        elif what == "lm":
            lm(*arg)
        else:
            names[what](*arg)

    i = loc_count[0]
    cp = pltpu.make_async_copy(lnrow_v, ln_hbm, loc_sems.at[i])
    cp.start()
    outs.append(cp)
    for cp in outs:
        cp.wait()

    def drain_talk():
        for l in started["talk"]:
            l.sent()

    talkers(drain_talk)

    def drain_quiet():
        for l in started["quiet"]:
            l.sent()

    quiet(drain_quiet)


def make_order(n, n_lm, lm_chunks, n_tiles):
    seq = ["first_send", "first_relay", "second_send", "own_block",
           "spread_first", "spread_forward", "spread_last", "arrive"]
    order = []
    todo = {k: list(seq) for k in range(n)}

    def advance(k):
        if todo[k]:
            order.append((todo[k].pop(0), k))

    for k in range(n):
        order.append(("mlp", k))
        if k == 0:
            order.append(("meet",))
        order.append(("pair_send", k))
        for j in range(k):
            advance(j)
    need = lm_chunks[0]
    while any(todo[k] for k in need):
        for k in range(n):
            advance(k)
            if not any(todo[j] for j in need):
                break
    tails = {}
    tseq = ["tail_one", "tail_two", "tail_three", "tail_done"]

    def service():
        for k in range(n):
            advance(k)
        for l in list(tails):
            if tails[l]:
                order.append((tails[l].pop(0), l))

    order.append(("ids",))
    order.append(("weights",))
    half = n_tiles // 2
    for l in range(n_lm):
        while any(todo[k] for k in lm_chunks[l]):
            for k in range(n):
                advance(k)
        order.append(("normalize", l))
        order.append(("lm", l, 0, half))
        service()
        order.append(("lm", l, half, n_tiles))
        order.append(("tail_pair", l))
        service()
        tails[l] = list(tseq)
    while any(tails.values()):
        for l in tails:
            if tails[l]:
                order.append((tails[l].pop(0), l))
    return order


def plan_chunks(batch):
    rows = ROWS_LM
    chunks = [(i * rows, rows) for i in range(batch // rows)]
    return chunks, [[i] for i in range(len(chunks))]


def solution(mesh):
    n_tp = mesh.shape["tp"]
    q = math.isqrt(n_tp // CORES)

    def local_step(resid_in, cand_ids, ln_mlp, wi_gate, wi_lin, w_out, ln_final, w_lm):
        batch, width = resid_in.shape
        inner = wi_gate.shape[1]
        vocab = w_lm.shape[1]
        cands = cand_ids.shape[1]
        chunks, lm_chunks = plan_chunks(batch)
        n_tiles = -(-vocab // TILE)
        w_parts = 4
        cfg = dict(q=q, chunks=chunks, lm=lm_chunks, w_parts=w_parts,
                   order=make_order(len(chunks), len(lm_chunks), lm_chunks, n_tiles))
        ns = 2 if NORTH else 1
        f32 = jnp.float32
        blocks = q * q
        bufs, tails = [], []
        for _, rows in chunks:
            r2 = rows // 2
            hr = r2 // 2
            bufs.append((
                pltpu.VMEM((2, blocks, r2, LANES), f32),
                pltpu.VMEM((ns, blocks, r2, LANES), f32),
                pltpu.VMEM((ns, 2, q, hr, LANES), f32),
                pltpu.VMEM((ns, 2, q, hr, LANES), f32),
                pltpu.VMEM((ns, 2, q, hr, LANES), f32),
                pltpu.VMEM((ns, q, r2, LANES), f32),
                pltpu.VMEM((ns, q - 1, r2, LANES), f32),
                pltpu.VMEM((2, blocks, r2, LANES), f32),
            ))
        rt = ROWS_LM // 2 + 8
        for _ in lm_chunks:
            tails.append((
                pltpu.VMEM((2, rt, cands), f32),
                pltpu.VMEM((ns, rt, cands), f32),
                pltpu.VMEM((ns, q, rt, cands), f32),
                pltpu.VMEM((ns, q, rt, cands), f32),
                pltpu.VMEM((2, rt, cands), f32),
            ))
        n_links = len(chunks) * (ns * 25 + 2) + len(lm_chunks) * (ns * 10 + 2)
        n_loc = len(chunks) + len(lm_chunks) + w_parts + 6
        hbm = pl.BlockSpec(memory_space=pltpu.HBM)
        vmem = pl.BlockSpec(memory_space=pltpu.VMEM)
        scratch = [
            pltpu.VMEM((batch, width), jnp.bfloat16),
            pltpu.VMEM((batch, cands), jnp.int32),
            pltpu.VMEM((width, inner), jnp.bfloat16),
            pltpu.VMEM((width, inner), jnp.bfloat16),
            pltpu.VMEM((inner, width), jnp.bfloat16),
            pltpu.VMEM((width, vocab), jnp.bfloat16),
            pltpu.VMEM((ROWS_LM, width), jnp.bfloat16),
            pltpu.VMEM((2, ROWS_LM, TILE), f32),
            pltpu.VMEM((4, ROWS_LM, LANES), f32),
            pltpu.VMEM((2, ROWS_LM // 2, LANES), f32),
            pltpu.VMEM((len(lm_chunks), LANES), f32),
            pltpu.VMEM((batch, cands), f32),
            tuple(bufs),
            tuple(tails),
            pltpu.SemaphoreType.DMA((n_links,)),
            pltpu.SemaphoreType.DMA((n_links,)),
            pltpu.SemaphoreType.DMA((n_loc,)),
        ]
        log_probs, log_norm = pl.pallas_call(
            functools.partial(fused, cfg),
            out_shape=(
                jax.ShapeDtypeStruct((batch, cands), f32),
                jax.ShapeDtypeStruct((len(lm_chunks), LANES), f32),
            ),
            in_specs=[hbm, hbm, vmem, hbm, hbm, hbm, vmem, hbm],
            out_specs=(hbm, hbm),
            scratch_shapes=scratch,
            compiler_params=pltpu.CompilerParams(
                collective_id=0, has_side_effects=True, vmem_limit_bytes=67_043_328),
            name="fused",
        )(resid_in, cand_ids, ln_mlp.reshape(1, width), wi_gate, wi_lin, w_out,
          ln_final.reshape(1, width), w_lm)
        return log_probs, log_norm.reshape(batch)

    in_specs = (P("dp", None), P("dp", None), P(None), P(None, "tp"), P(None, "tp"), P("tp", None), P(None), P(None, "tp"))
    return jax.shard_map(local_step, mesh=mesh, in_specs=in_specs, out_specs=(P("dp", None), P("dp")), check_vma=False)
```

```python
import functools
import math

import jax
import jax.numpy as jnp
from jax import lax
from jax.experimental import pallas as pl
from jax.experimental.pallas import tpu as pltpu
from jax.sharding import PartitionSpec as P

EPS = 1e-6
LANES = 128
CORES = 2
MESH = pl.DeviceIdType.MESH
NEG = float("-inf")

NORTH = False
ROWS_LM = 256
ROWS_COMM = 128
TILE = 1024
GROUP = 64
TRANS_B = (((1,), (1,)), ((), ()))


def rms_rows(wide, scale):
    mean_sq = jnp.mean(wide * wide, axis=-1, keepdims=True)
    return (wide * lax.rsqrt(mean_sq + EPS) * scale).astype(jnp.bfloat16)


def log_add(parts):
    top = functools.reduce(jnp.maximum, parts)
    total = functools.reduce(jnp.add, [jnp.exp(p - top) for p in parts])
    return top + jnp.log(total)


class Link:
    def __init__(self, src, dst, send, recv, to):
        self.args = dict(
            src_ref=src, dst_ref=dst, send_sem=send, recv_sem=recv,
            device_id={"tp": to}, device_id_type=MESH,
        )

    def make(self):
        return pltpu.make_async_remote_copy(**self.args)

    def start(self):
        self.make().start()

    def sent(self):
        self.make().wait_send()

    def came(self):
        self.make().wait_recv()


def fused(cfg, x_hbm, ids_hbm, lnm_ref, wg_hbm, wl_hbm, wo_hbm, lnf_ref, w_hbm,
          lp_hbm, ln_hbm,
          x_v, ids_v, wg_v, wl_v, wo_v, w_v, z_v, lg_v, st_v, lnrow_v, ob_v,
          bufs, tails, send_sems, recv_sems, loc_sems):
    q, chunks, lm_chunks = cfg["q"], cfg["chunks"], cfg["lm"]
    me = lax.axis_index("tp")
    core = lax.rem(me, CORES)
    x = lax.rem(me // CORES, q)
    y = me // (CORES * q)
    sibling = me + 1 - 2 * core
    vocab = w_v.shape[0]
    ndev_side = q

    if NORTH:
        slots = [0, 1]
        half_of = [0, 1]
        speak = 1
    else:
        slots = [0]
        half_of = [core]
        speak = core

    def coords(s):
        if NORTH:
            return (x, y) if s == 0 else (y, x)
        a = jnp.where(core == 0, x, y)
        b = jnp.where(core == 0, y, x)
        return a, b

    def device(s, a, b):
        if NORTH:
            col, row = (a, b) if s == 0 else (b, a)
            return (row * q + col) * CORES + 1
        col = jnp.where(core == 0, a, b)
        row = jnp.where(core == 0, b, a)
        return (row * q + col) * CORES + core

    def step(v, d):
        return lax.rem(v + d + q, q)

    counter = [0]
    started = {"all": [], "talk": [], "quiet": []}

    def link(src, dst, to, who="talk"):
        i = counter[0]
        counter[0] += 1
        made = Link(src, dst, send_sems.at[i], recv_sems.at[i], to)
        started[who].append(made)
        return made

    def talkers(fn):
        if NORTH:
            pl.when(core == 1)(fn)
        else:
            fn()

    def quiet(fn):
        if NORTH:
            pl.when(core == 0)(fn)

    loads = {}
    loc_count = [0]

    def load(name, src, dst):
        i = loc_count[0]
        loc_count[0] += 1
        cp = pltpu.make_async_copy(src, dst, loc_sems.at[i])
        loads[name] = cp
        cp.start()

    off0, rows0 = chunks[0]
    load("x0", x_hbm.at[pl.ds(off0, rows0), :], x_v.at[pl.ds(off0, rows0), :])
    load("wg", wg_hbm, wg_v)
    load("wl", wl_hbm, wl_v)
    load("wo", wo_hbm, wo_v)
    for k, (off, rows) in enumerate(chunks[1:], 1):
        load(f"x{k}", x_hbm.at[pl.ds(off, rows), :], x_v.at[pl.ds(off, rows), :])
    load("ids", ids_hbm, ids_v)
    parts = cfg["w_parts"]
    for i in range(parts):
        band = pl.ds(i * TILE, min(TILE, vocab - i * TILE))
        load(f"w{i}", w_hbm.at[band, :], w_v.at[band, :])

    barrier = pltpu.get_barrier_semaphore()

    def greet(to):
        pl.semaphore_signal(barrier, inc=1, device_id={"tp": to}, device_id_type=MESH)

    greet(sibling)

    def greet_far():
        a, b = coords(0)
        for d in range(1, q):
            greet(device(0, step(a, d), b))
            greet(device(0, a, step(b, d)))

    talkers(greet_far)

    def meet():
        if NORTH:
            pl.when(core == 1)(lambda: pl.semaphore_wait(barrier, 1 + 2 * (q - 1)))
            pl.when(core == 0)(lambda: pl.semaphore_wait(barrier, 1))
        else:
            pl.semaphore_wait(barrier, 1 + 2 * (q - 1))

    scale_mlp = lnm_ref[...].astype(jnp.float32).reshape(1, -1)
    scale_fin = lnf_ref[...].astype(jnp.float32).reshape(1, -1)

    plans = []
    for k, (off, rows) in enumerate(chunks):
        r2 = rows // 2
        hr = r2 // 2
        px, dr, rl, dc, cb, bs, pr, xb = bufs[k]
        plan = {"slots": []}
        if NORTH:
            plan["pair"] = [link(px.at[h], dr.at[h], sibling, "quiet") for h in (0, 1)]
        else:
            plan["pair"] = [link(px.at[1 - core], dr.at[0], sibling)]
        for s in slots:
            a, b = coords(s)
            h = half_of[s]
            up, down, far = step(a, 1), step(a, -1), step(a, 2)
            to_up, to_down = device(s, up, b), device(s, down, b)
            lo, hi = pl.ds(0, hr), pl.ds(hr, hr)

            def grp(v):
                return pl.ds(v * q, q)

            e = {}
            e["relay"] = [
                link(dr.at[s, grp(far), lo, :], rl.at[s, 0], to_up),
                link(dr.at[s, grp(far), hi, :], rl.at[s, 1], to_down),
            ]
            e["direct"] = [
                link(dr.at[s, grp(down), lo, :], dc.at[s, 0], to_down),
                link(dr.at[s, grp(up), hi, :], dc.at[s, 1], to_up),
            ]
            e["comb"] = [
                link(rl.at[s, 0], cb.at[s, 0], to_up),
                link(rl.at[s, 1], cb.at[s, 1], to_down),
            ]
            e["second"] = [
                link(bs.at[s, step(b, d)], pr.at[s, d - 1], device(s, a, step(b, d)))
                for d in range(1, q)
            ]
            own = xb.at[h, a * q + b]
            e["spread2"] = [link(own, own, device(s, a, step(b, d))) for d in range(1, q)]
            mine_lo = xb.at[h, grp(a), lo, :]
            mine_hi = xb.at[h, grp(a), hi, :]
            e["up"] = [link(mine_lo, mine_lo, to_up), link(mine_hi, mine_hi, to_up)]
            e["down"] = [link(mine_lo, mine_lo, to_down), link(mine_hi, mine_hi, to_down)]
            fwd_lo = xb.at[h, grp(down), lo, :]
            fwd_hi = xb.at[h, grp(up), hi, :]
            e["fwd"] = [link(fwd_lo, fwd_lo, to_up), link(fwd_hi, fwd_hi, to_down)]
            e["pass"] = [
                link(xb.at[h, grp(step(a, d))], xb.at[h, grp(step(a, d))], sibling)
                for d in range(q)
            ]
            plan["slots"].append(e)
        plans.append(plan)

    def mlp(k):
        off, rows = chunks[k]
        px = bufs[k][0]
        r2 = rows // 2
        loads[f"x{k}"].wait()
        wide = x_v[pl.ds(off, rows), :].astype(jnp.float32)
        normed = rms_rows(wide, scale_mlp)
        if k == 0:
            loads["wg"].wait()
            loads["wl"].wait()
        gate = lax.dot_general(normed, wg_v[...], TRANS_B, preferred_element_type=jnp.float32)
        lin = lax.dot_general(normed, wl_v[...], TRANS_B, preferred_element_type=jnp.float32)
        hidden = (jax.nn.gelu(gate, approximate=True) * lin).astype(jnp.bfloat16)
        if k == 0:
            loads["wo"].wait()
        part = jnp.dot(hidden, wo_v[...], preferred_element_type=jnp.float32)
        for h in range(2):
            for j in range(q * q):
                px[h, j] = part[h * r2:(h + 1) * r2, j * LANES:(j + 1) * LANES]

    def pair_send(k):
        def go():
            for l in plans[k]["pair"]:
                l.start()
        if NORTH:
            quiet(go)
        else:
            go()

    def first_send(k):
        px, dr = bufs[k][0], bufs[k][1]

        def go():
            for l in plans[k]["pair"]:
                l.came()
            for s in slots:
                a, _ = coords(s)
                h = half_of[s]
                e = plans[k]["slots"][s]
                for d in (2, 1, 3, 0):
                    g = pl.ds(step(a, d) * q, q)
                    dr[s, g] = dr[s, g] + px[h, g]
                    if d == 2:
                        for l in e["relay"]:
                            l.start()
                    if d == 3:
                        for l in e["direct"]:
                            l.start()
        talkers(go)

    def first_relay(k):
        _, dr, rl = bufs[k][:3]
        hr = chunks[k][1] // 4

        def go():
            for s in slots:
                a, _ = coords(s)
                e = plans[k]["slots"][s]
                for i, d in ((0, 1), (1, -1)):
                    e["relay"][i].came()
                    g = pl.ds(step(a, d) * q, q)
                    rl[s, i] = rl[s, i] + dr[s, g, i * hr:(i + 1) * hr, :]
                    e["comb"][i].start()
        talkers(go)

    def second_send(k):
        _, dr, _, dc, cb, bs = bufs[k][:6]
        hr = chunks[k][1] // 4

        def go():
            for s in slots:
                a, _ = coords(s)
                e = plans[k]["slots"][s]
                g = pl.ds(a * q, q)
                for i in range(2):
                    e["direct"][i].came()
                    e["comb"][i].came()
                    part = slice(i * hr, (i + 1) * hr)
                    bs[s, :, part, :] = dr[s, g, part, :] + dc[s, i] + cb[s, i]
                for l in e["second"]:
                    l.start()
        talkers(go)

    def own_block(k):
        off, rows = chunks[k]
        r2 = rows // 2
        bs, pr, xb = bufs[k][5:]

        def go():
            for s in slots:
                a, b = coords(s)
                h = half_of[s]
                e = plans[k]["slots"][s]
                for l in e["second"]:
                    l.came()
                total = bs[s, b]
                for d in range(q - 1):
                    total = total + pr[s, d]
                col = pl.ds(pl.multiple_of((a * q + b) * LANES, LANES), LANES)
                row = pl.ds(pl.multiple_of(off + h * r2, 16), r2)
                resid = x_v[row, col].astype(jnp.float32)
                xb[h, a * q + b] = (resid + total).astype(jnp.bfloat16).astype(jnp.float32)
                for l in e["spread2"]:
                    l.start()
        talkers(go)

    def spread_first(k):
        def go():
            for s in slots:
                e = plans[k]["slots"][s]
                for l in e["spread2"]:
                    l.came()
                e["up"][0].start()
                e["down"][1].start()
                e["up"][1].start()
                e["down"][0].start()
                e["pass"][0].start()
        talkers(go)

    def spread_forward(k):
        def go():
            for s in slots:
                e = plans[k]["slots"][s]
                e["up"][0].came()
                e["fwd"][0].start()
                e["down"][1].came()
                e["fwd"][1].start()
        talkers(go)

    def spread_last(k):
        def go():
            for s in slots:
                e = plans[k]["slots"][s]
                e["up"][1].came()
                e["pass"][q - 1].start()
                e["down"][0].came()
                e["pass"][1].start()
                for l in e["fwd"]:
                    l.came()
                e["pass"][2].start()
        talkers(go)

    def arrive(k):
        def go():
            for s in slots:
                for l in plans[k]["slots"][s]["pass"]:
                    l.came()
        if NORTH:
            quiet(go)
        else:
            go()

    def normalize(l):
        first = lm_chunks[l]
        base = chunks[first[0]][0]
        for k in first:
            off, rows = chunks[k]
            r2 = rows // 2
            xb = bufs[k][7]
            for h in range(2):
                sq = None
                for j in range(q * q):
                    v = xb[h, j]
                    sq = v * v if sq is None else sq + v * v
                mean_sq = jnp.sum(sq, axis=-1, keepdims=True) * (1.0 / (q * q * LANES))
                inv = jnp.broadcast_to(lax.rsqrt(mean_sq + EPS), (r2, LANES))
                for j in range(q * q):
                    cols = slice(j * LANES, (j + 1) * LANES)
                    z_v[off - base + h * r2:off - base + (h + 1) * r2, cols] = (
                        xb[h, j] * inv * scale_fin[:, cols]
                    ).astype(jnp.bfloat16)

    n_tiles = -(-vocab // TILE)

    def lm(l, t0, t1):
        rows = ROWS_LM
        base = chunks[lm_chunks[l][0]][0]
        for t in range(t0, t1):
            a = t * TILE
            wd = min(TILE, vocab - a)
            slot = t % 2
            lg_v[slot, :, :wd] = lax.dot_general(
                z_v[...], w_v[a:a + wd, :], TRANS_B, preferred_element_type=jnp.float32)
            nv = -(-wd // LANES)
            for g in range(0, rows, GROUP):
                at = slice(g, g + GROUP)
                xs = [lg_v[slot, at, j * LANES:(j + 1) * LANES] for j in range(nv)]
                if wd % LANES:
                    pos = lax.broadcasted_iota(jnp.int32, (GROUP, LANES), 1)
                    xs[-1] = jnp.where(pos < wd % LANES, xs[-1], NEG)
                new = functools.reduce(jnp.maximum, xs)
                acc = None
                if t > 0:
                    old = st_v[0, at, :]
                    new = jnp.maximum(old, new)
                    acc = st_v[1, at, :] * jnp.exp(old - new)
                for v in xs:
                    ev = jnp.exp(v - new)
                    acc = ev if acc is None else acc + ev
                st_v[0, at, :] = new
                st_v[1, at, :] = acc
                for c in range(2):
                    loc = ids_v[base + g:base + g + GROUP, c * LANES:(c + 1) * LANES] - me * vocab
                    inside = (loc >= 0) & (loc < vocab)
                    chunk = jnp.where(inside, lax.shift_right_arithmetic(loc, 7), -1)
                    lane = loc & (LANES - 1)
                    pick = st_v[2 + c, at, :] if t > 0 else jnp.zeros((GROUP, LANES), jnp.float32)
                    for j in range(nv):
                        got = jnp.take_along_axis(xs[j], lane, axis=1, mode="promise_in_bounds")
                        pick = jnp.where(chunk == a // LANES + j, got, pick)
                    st_v[2 + c, at, :] = pick
        if t1 < n_tiles:
            return
        top, total = st_v[0], st_v[1]
        peak = jnp.max(top, axis=-1, keepdims=True)
        mass = jnp.sum(total * jnp.exp(top - peak), axis=-1, keepdims=True)
        part = jnp.broadcast_to(peak + jnp.log(mass), (rows, LANES))
        tp = tails[l][0]
        for h in range(2):
            for c in range(2):
                cols = slice(c * LANES, (c + 1) * LANES)
                tp[h, 0:r2, cols] = st_v[2 + c, h * r2:(h + 1) * r2, :]
            tp[h, r2:r2 + 8, :] = part.T[0:8, :]

    r2 = ROWS_LM // 2
    tplans = []
    for l in range(len(lm_chunks)):
        tp, t1r, t2r, t3r, tc = tails[l]
        plan = {"slots": []}
        if NORTH:
            plan["pair"] = [link(tp.at[h], t1r.at[h], sibling, "quiet") for h in (0, 1)]
        else:
            plan["pair"] = [link(tp.at[1 - core], t1r.at[0], sibling)]
        for s in slots:
            a, b = coords(s)
            h = half_of[s]
            plan["slots"].append({
                "one": [link(t2r.at[s, a], t2r.at[s, a], device(s, step(a, d), b)) for d in range(1, q)],
                "two": [link(t3r.at[s, b], t3r.at[s, b], device(s, a, step(b, d))) for d in range(1, q)],
                "back": [link(tc.at[h], tc.at[h], sibling)],
            })
        tplans.append(plan)

    def join(refs, out):
        total = functools.reduce(jnp.add, [r[0:r2, :] for r in refs])
        out[0:r2, :] = total
        out[r2:r2 + 8, :] = log_add([r[r2:r2 + 8, :] for r in refs])

    def tail_pair(l):
        def go():
            for k in tplans[l]["pair"]:
                k.start()
        if NORTH:
            quiet(go)
        else:
            go()

    def tail_one(l):
        tp, t1r, t2r = tails[l][:3]

        def go():
            for k in tplans[l]["pair"]:
                k.came()
            for s in slots:
                join([tp.at[half_of[s]], t1r.at[s]], t2r.at[s, coords(s)[0]])
                for k in tplans[l]["slots"][s]["one"]:
                    k.start()
        talkers(go)

    def tail_two(l):
        t2r, t3r = tails[l][2:4]

        def go():
            for s in slots:
                for k in tplans[l]["slots"][s]["one"]:
                    k.came()
                join([t2r.at[s, d] for d in range(q)], t3r.at[s, coords(s)[1]])
                for k in tplans[l]["slots"][s]["two"]:
                    k.start()
        talkers(go)

    def tail_three(l):
        t3r, tc = tails[l][3:5]

        def go():
            for s in slots:
                for k in tplans[l]["slots"][s]["two"]:
                    k.came()
                join([t3r.at[s, d] for d in range(q)], tc.at[half_of[s]])
                for k in tplans[l]["slots"][s]["back"]:
                    k.start()
        talkers(go)

    outs = []

    def tail_done(l):
        tc = tails[l][4]

        def go():
            for s in slots:
                for k in tplans[l]["slots"][s]["back"]:
                    k.came()
        if NORTH:
            quiet(go)
        else:
            go()
        base = chunks[lm_chunks[l][0]][0]
        row = tc[0, r2:r2 + 1, :]
        lnrow_v[l:l + 1, :] = row
        lse = jnp.broadcast_to(row, (LANES, ROWS_LM)).T
        for h in range(2):
            for c in range(2):
                cols = slice(c * LANES, (c + 1) * LANES)
                ob_v[base + h * r2:base + (h + 1) * r2, cols] = (
                    tc[h, 0:r2, cols] - lse[h * r2:(h + 1) * r2, :]
                )
        i = loc_count[0]
        loc_count[0] += 1
        cp = pltpu.make_async_copy(
            ob_v.at[base:base + ROWS_LM, :], lp_hbm.at[base:base + ROWS_LM, :], loc_sems.at[i])
        cp.start()
        outs.append(cp)

    stages = [mlp, pair_send, first_send, first_relay, second_send, own_block,
              spread_first, spread_forward, spread_last]
    names = {f.__name__: f for f in stages}
    names.update({f.__name__: f for f in (arrive, normalize, tail_pair, tail_one, tail_two, tail_three, tail_done)})
    for item in cfg["order"]:
        what, arg = item[0], item[1:]
        with jax.named_scope("_".join(str(v) for v in item)):
            if what == "meet":
                meet()
            elif what == "weights":
                if arg[0] < parts:
                    loads[f"w{arg[0]}"].wait()
            elif what == "ids":
                loads["ids"].wait()
            elif what == "lm":
                lm(*arg)
            else:
                names[what](*arg)

    i = loc_count[0]
    cp = pltpu.make_async_copy(lnrow_v, ln_hbm, loc_sems.at[i])
    cp.start()
    outs.append(cp)
    for cp in outs:
        cp.wait()

    def drain_talk():
        for l in started["talk"]:
            l.sent()

    talkers(drain_talk)

    def drain_quiet():
        for l in started["quiet"]:
            l.sent()

    quiet(drain_quiet)


def make_order(n, n_lm, lm_chunks, n_tiles):
    seq = ["first_send", "first_relay", "second_send", "own_block",
           "spread_first", "spread_forward", "spread_last", "arrive"]
    order = []
    todo = {k: list(seq) for k in range(n)}

    def advance(k):
        if todo[k]:
            order.append((todo[k].pop(0), k))

    for k in range(n):
        order.append(("mlp", k))
        if k == 0:
            order.append(("meet",))
        order.append(("pair_send", k))
        for j in range(k):
            advance(j)
    need = lm_chunks[0]
    while any(todo[k] for k in need):
        for k in range(n):
            advance(k)
            if not any(todo[j] for j in need):
                break
    order.append(("ids",))
    tail = []
    for l in range(n_lm):
        while any(todo[k] for k in lm_chunks[l]):
            for k in range(n):
                advance(k)
        order.append(("normalize", l))
        for t in range(0, n_tiles, 2):
            if l == 0:
                order.append(("weights", t))
                order.append(("weights", t + 1))
            order.append(("lm", l, t, min(t + 2, n_tiles)))
            if t + 2 < n_tiles:
                for k in range(n):
                    advance(k)
                if tail:
                    order.append(tail.pop(0))
        order.append(("tail_pair", l))
        tail += [("tail_one", l), ("tail_two", l), ("tail_three", l), ("tail_done", l)]
    order += tail
    return order


def plan_chunks(batch):
    rows = ROWS_COMM
    chunks = [(i * rows, rows) for i in range(batch // rows)]
    per = ROWS_LM // rows
    return chunks, [list(range(i, i + per)) for i in range(0, len(chunks), per)]


def solution(mesh):
    n_tp = mesh.shape["tp"]
    q = math.isqrt(n_tp // CORES)

    def local_step(resid_in, cand_ids, ln_mlp, wi_gate, wi_lin, w_out, ln_final, w_lm):
        batch, width = resid_in.shape
        inner = wi_gate.shape[1]
        vocab = w_lm.shape[1]
        w_parts = -(-vocab // TILE)
        cands = cand_ids.shape[1]
        chunks, lm_chunks = plan_chunks(batch)
        n_tiles = -(-vocab // TILE)
        cfg = dict(q=q, chunks=chunks, lm=lm_chunks, w_parts=w_parts,
                   order=make_order(len(chunks), len(lm_chunks), lm_chunks, n_tiles))
        ns = 2 if NORTH else 1
        f32 = jnp.float32
        blocks = q * q
        bufs, tails = [], []
        for _, rows in chunks:
            r2 = rows // 2
            hr = r2 // 2
            bufs.append((
                pltpu.VMEM((2, blocks, r2, LANES), f32),
                pltpu.VMEM((ns, blocks, r2, LANES), f32),
                pltpu.VMEM((ns, 2, q, hr, LANES), f32),
                pltpu.VMEM((ns, 2, q, hr, LANES), f32),
                pltpu.VMEM((ns, 2, q, hr, LANES), f32),
                pltpu.VMEM((ns, q, r2, LANES), f32),
                pltpu.VMEM((ns, q - 1, r2, LANES), f32),
                pltpu.VMEM((2, blocks, r2, LANES), f32),
            ))
        rt = ROWS_LM // 2 + 8
        for _ in lm_chunks:
            tails.append((
                pltpu.VMEM((2, rt, cands), f32),
                pltpu.VMEM((ns, rt, cands), f32),
                pltpu.VMEM((ns, q, rt, cands), f32),
                pltpu.VMEM((ns, q, rt, cands), f32),
                pltpu.VMEM((2, rt, cands), f32),
            ))
        n_links = len(chunks) * (ns * 25 + 2) + len(lm_chunks) * (ns * 10 + 2)
        n_loc = len(chunks) + len(lm_chunks) + w_parts + 6
        hbm = pl.BlockSpec(memory_space=pltpu.HBM)
        vmem = pl.BlockSpec(memory_space=pltpu.VMEM)
        scratch = [
            pltpu.VMEM((batch, width), jnp.bfloat16),
            pltpu.VMEM((batch, cands), jnp.int32),
            pltpu.VMEM((inner, width), jnp.bfloat16),
            pltpu.VMEM((inner, width), jnp.bfloat16),
            pltpu.VMEM((inner, width), jnp.bfloat16),
            pltpu.VMEM((vocab, width), jnp.bfloat16),
            pltpu.VMEM((ROWS_LM, width), jnp.bfloat16),
            pltpu.VMEM((2, ROWS_LM, TILE), f32),
            pltpu.VMEM((4, ROWS_LM, LANES), f32),
            pltpu.VMEM((len(lm_chunks), ROWS_LM), f32),
            pltpu.VMEM((batch, cands), f32),
            tuple(bufs),
            tuple(tails),
            pltpu.SemaphoreType.DMA((n_links,)),
            pltpu.SemaphoreType.DMA((n_links,)),
            pltpu.SemaphoreType.DMA((n_loc,)),
        ]
        log_probs, log_norm = pl.pallas_call(
            functools.partial(fused, cfg),
            out_shape=(
                jax.ShapeDtypeStruct((batch, cands), f32),
                jax.ShapeDtypeStruct((len(lm_chunks), ROWS_LM), f32),
            ),
            in_specs=[hbm, hbm, vmem, hbm, hbm, hbm, vmem, hbm],
            out_specs=(hbm, hbm),
            scratch_shapes=scratch,
            compiler_params=pltpu.CompilerParams(
                collective_id=0, has_side_effects=True, vmem_limit_bytes=67_043_328),
            name="fused",
        )(resid_in, cand_ids, ln_mlp, wi_gate.T, wi_lin.T, w_out, ln_final, w_lm.T)
        return log_probs, log_norm.reshape(batch)

    in_specs = (P("dp", None), P("dp", None), P(None), P(None, "tp"), P(None, "tp"), P("tp", None), P(None), P(None, "tp"))
    return jax.shard_map(local_step, mesh=mesh, in_specs=in_specs, out_specs=(P("dp", None), P("dp")), check_vma=False)
```

```python
import functools
import math

import jax
import jax.numpy as jnp
from jax import lax
from jax.experimental import pallas as pl
from jax.experimental.pallas import tpu as pltpu
from jax.sharding import PartitionSpec as P

EPS = 1e-6
LANES = 128
CORES = 2
MESH = pl.DeviceIdType.MESH
NEG = float("-inf")

NORTH = False
ROWS_LM = 256
ROWS_COMM = 128
TILE = 1024
GROUP = 64
TRANS_B = (((1,), (1,)), ((), ()))


def rms_rows(wide, scale):
    mean_sq = jnp.mean(wide * wide, axis=-1, keepdims=True)
    return (wide * lax.rsqrt(mean_sq + EPS) * scale).astype(jnp.bfloat16)


def log_add(parts):
    top = functools.reduce(jnp.maximum, parts)
    total = functools.reduce(jnp.add, [jnp.exp(p - top) for p in parts])
    return top + jnp.log(total)


class Link:
    def __init__(self, src, dst, send, recv, to):
        self.args = dict(
            src_ref=src, dst_ref=dst, send_sem=send, recv_sem=recv,
            device_id={"tp": to}, device_id_type=MESH,
        )

    def make(self):
        return pltpu.make_async_remote_copy(**self.args)

    def start(self):
        self.make().start()

    def sent(self):
        self.make().wait_send()

    def came(self):
        self.make().wait_recv()


def fused(cfg, x_hbm, ids_hbm, lnm_ref, wg_hbm, wl_hbm, wo_hbm, lnf_ref, w_hbm,
          lp_hbm, ln_hbm,
          x_v, ids_v, wg_v, wl_v, wo_v, w_v, z_v, lg_v, st_v, lnrow_v, ob_v,
          bufs, tails, send_sems, recv_sems, loc_sems):
    q, chunks, lm_chunks = cfg["q"], cfg["chunks"], cfg["lm"]
    me = lax.axis_index("tp")
    core = lax.rem(me, CORES)
    x = lax.rem(me // CORES, q)
    y = me // (CORES * q)
    sibling = me + 1 - 2 * core
    vocab = w_v.shape[0]
    ndev_side = q

    if NORTH:
        slots = [0, 1]
        half_of = [0, 1]
        speak = 1
    else:
        slots = [0]
        half_of = [core]
        speak = core

    def coords(s):
        if NORTH:
            return (x, y) if s == 0 else (y, x)
        a = jnp.where(core == 0, x, y)
        b = jnp.where(core == 0, y, x)
        return a, b

    def device(s, a, b):
        if NORTH:
            col, row = (a, b) if s == 0 else (b, a)
            return (row * q + col) * CORES + 1
        col = jnp.where(core == 0, a, b)
        row = jnp.where(core == 0, b, a)
        return (row * q + col) * CORES + core

    def step(v, d):
        return lax.rem(v + d + q, q)

    far_first = sorted(range(1, q), key=lambda d: -min(d, q - d))

    counter = [0]
    started = {"all": [], "talk": [], "quiet": []}

    def link(src, dst, to, who="talk"):
        i = counter[0]
        counter[0] += 1
        made = Link(src, dst, send_sems.at[i], recv_sems.at[i], to)
        started[who].append(made)
        return made

    def talkers(fn):
        if NORTH:
            pl.when(core == 1)(fn)
        else:
            fn()

    def quiet(fn):
        if NORTH:
            pl.when(core == 0)(fn)

    loads = {}
    loc_count = [0]

    def load(name, src, dst):
        i = loc_count[0]
        loc_count[0] += 1
        cp = pltpu.make_async_copy(src, dst, loc_sems.at[i])
        loads[name] = cp
        cp.start()

    off0, rows0 = chunks[0]
    load("x0", x_hbm.at[pl.ds(off0, rows0), :], x_v.at[pl.ds(off0, rows0), :])
    load("wg", wg_hbm, wg_v)
    load("wl", wl_hbm, wl_v)
    load("wo", wo_hbm, wo_v)
    for k, (off, rows) in enumerate(chunks[1:], 1):
        load(f"x{k}", x_hbm.at[pl.ds(off, rows), :], x_v.at[pl.ds(off, rows), :])
    load("ids", ids_hbm, ids_v)
    parts = cfg["w_parts"]
    for i in range(parts):
        band = pl.ds(i * TILE, min(TILE, vocab - i * TILE))
        load(f"w{i}", w_hbm.at[band, :], w_v.at[band, :])

    barrier = pltpu.get_barrier_semaphore()

    def greet(to):
        pl.semaphore_signal(barrier, inc=1, device_id={"tp": to}, device_id_type=MESH)

    greet(sibling)

    def greet_far():
        a, b = coords(0)
        for d in range(1, q):
            greet(device(0, step(a, d), b))
            greet(device(0, a, step(b, d)))

    talkers(greet_far)

    def meet():
        if NORTH:
            pl.when(core == 1)(lambda: pl.semaphore_wait(barrier, 1 + 2 * (q - 1)))
            pl.when(core == 0)(lambda: pl.semaphore_wait(barrier, 1))
        else:
            pl.semaphore_wait(barrier, 1 + 2 * (q - 1))

    scale_mlp = lnm_ref[...].astype(jnp.float32).reshape(1, -1)
    scale_fin = lnf_ref[...].astype(jnp.float32).reshape(1, -1)

    plans = []
    for k, (off, rows) in enumerate(chunks):
        r2 = rows // 2
        px, dr, rl, bs, pr, xb = bufs[k]
        plan = {"slots": []}
        if NORTH:
            plan["pair"] = [link(px.at[h], dr.at[h], sibling, "quiet") for h in (0, 1)]
        else:
            plan["pair"] = [link(px.at[1 - core], dr.at[0], sibling)]
        for s in slots:
            a, b = coords(s)
            h = half_of[s]

            def grp(v):
                return pl.ds(v * q, q)

            e = {}
            e["one"] = [
                link(dr.at[s, grp(step(a, d))], rl.at[s, d - 1], device(s, step(a, d), b))
                for d in range(1, q)
            ]
            e["second"] = [
                link(bs.at[s, step(b, d)], pr.at[s, d - 1], device(s, a, step(b, d)))
                for d in range(1, q)
            ]
            own = xb.at[h, a * q + b]
            e["spread2"] = [link(own, own, device(s, a, step(b, d))) for d in range(1, q)]
            mine = xb.at[h, grp(a)]
            e["wide"] = [link(mine, mine, device(s, step(a, d), b)) for d in range(1, q)]
            e["pass"] = [
                link(xb.at[h, grp(step(a, d))], xb.at[h, grp(step(a, d))], sibling)
                for d in range(q)
            ]
            plan["slots"].append(e)
        plans.append(plan)

    def mlp(k):
        off, rows = chunks[k]
        px = bufs[k][0]
        r2 = rows // 2
        loads[f"x{k}"].wait()
        wide = x_v[pl.ds(off, rows), :].astype(jnp.float32)
        normed = rms_rows(wide, scale_mlp)
        if k == 0:
            loads["wg"].wait()
            loads["wl"].wait()
        gate = lax.dot_general(normed, wg_v[...], TRANS_B, preferred_element_type=jnp.float32)
        lin = lax.dot_general(normed, wl_v[...], TRANS_B, preferred_element_type=jnp.float32)
        hidden = (jax.nn.gelu(gate, approximate=True) * lin).astype(jnp.bfloat16)
        if k == 0:
            loads["wo"].wait()
        part = jnp.dot(hidden, wo_v[...], preferred_element_type=jnp.float32)
        for h in range(2):
            for j in range(q * q):
                px[h, j] = part[h * r2:(h + 1) * r2, j * LANES:(j + 1) * LANES]

    def pair_send(k):
        def go():
            for l in plans[k]["pair"]:
                l.start()
        if NORTH:
            quiet(go)
        else:
            go()

    def first_send(k):
        px, dr = bufs[k][0], bufs[k][1]

        def go():
            for l in plans[k]["pair"]:
                l.came()
            for s in slots:
                a, _ = coords(s)
                h = half_of[s]
                e = plans[k]["slots"][s]
                for d in far_first + [0]:
                    g = pl.ds(step(a, d) * q, q)
                    dr[s, g] = dr[s, g] + px[h, g]
                    if d:
                        e["one"][d - 1].start()
        talkers(go)

    def second_send(k):
        _, dr, rl, bs = bufs[k][:4]

        def go():
            for s in slots:
                a, _ = coords(s)
                e = plans[k]["slots"][s]
                for l in e["one"]:
                    l.came()
                total = dr[s, pl.ds(a * q, q)]
                for d in range(q - 1):
                    total = total + rl[s, d]
                bs[s] = total
                for d in far_first:
                    e["second"][d - 1].start()
        talkers(go)

    def own_block(k):
        off, rows = chunks[k]
        r2 = rows // 2
        bs, pr, xb = bufs[k][3:]

        def go():
            for s in slots:
                a, b = coords(s)
                h = half_of[s]
                e = plans[k]["slots"][s]
                for l in e["second"]:
                    l.came()
                total = bs[s, b]
                for d in range(q - 1):
                    total = total + pr[s, d]
                col = pl.ds(pl.multiple_of((a * q + b) * LANES, LANES), LANES)
                row = pl.ds(pl.multiple_of(off + h * r2, 16), r2)
                resid = x_v[row, col].astype(jnp.float32)
                xb[h, a * q + b] = (resid + total).astype(jnp.bfloat16).astype(jnp.float32)
                for d in far_first:
                    e["spread2"][d - 1].start()
        talkers(go)

    def spread_first(k):
        def go():
            for s in slots:
                e = plans[k]["slots"][s]
                for l in e["spread2"]:
                    l.came()
                for d in far_first:
                    e["wide"][d - 1].start()
                e["pass"][0].start()
        talkers(go)

    def spread_last(k):
        def go():
            for s in slots:
                e = plans[k]["slots"][s]
                for d in reversed(far_first):
                    e["wide"][d - 1].came()
                    e["pass"][q - d].start()
        talkers(go)

    def arrive(k):
        def go():
            for s in slots:
                for l in plans[k]["slots"][s]["pass"]:
                    l.came()
        if NORTH:
            quiet(go)
        else:
            go()

    def normalize(l):
        first = lm_chunks[l]
        base = chunks[first[0]][0]
        for k in first:
            off, rows = chunks[k]
            r2 = rows // 2
            xb = bufs[k][5]
            for h in range(2):
                sq = None
                for j in range(q * q):
                    v = xb[h, j]
                    sq = v * v if sq is None else sq + v * v
                mean_sq = jnp.sum(sq, axis=-1, keepdims=True) * (1.0 / (q * q * LANES))
                inv = jnp.broadcast_to(lax.rsqrt(mean_sq + EPS), (r2, LANES))
                for j in range(q * q):
                    cols = slice(j * LANES, (j + 1) * LANES)
                    z_v[off - base + h * r2:off - base + (h + 1) * r2, cols] = (
                        xb[h, j] * inv * scale_fin[:, cols]
                    ).astype(jnp.bfloat16)

    n_tiles = -(-vocab // TILE)

    def logits_of(t):
        a = t * TILE
        wd = min(TILE, vocab - a)
        lg_v[t % 2, :, :wd] = lax.dot_general(
            z_v[...], w_v[a:a + wd, :], TRANS_B, preferred_element_type=jnp.float32)

    def fold(l, t):
        base = chunks[lm_chunks[l][0]][0]
        a = t * TILE
        wd = min(TILE, vocab - a)
        nv = -(-wd // LANES)
        for g in range(0, ROWS_LM, GROUP):
            at = slice(g, g + GROUP)
            xs = [lg_v[t % 2, at, j * LANES:(j + 1) * LANES] for j in range(nv)]
            if wd % LANES:
                pos = lax.broadcasted_iota(jnp.int32, (GROUP, LANES), 1)
                xs[-1] = jnp.where(pos < wd % LANES, xs[-1], NEG)
            new = functools.reduce(jnp.maximum, xs)
            acc = None
            if t > 0:
                old = st_v[0, at, :]
                new = jnp.maximum(old, new)
                acc = st_v[1, at, :] * jnp.exp(old - new)
            for v in xs:
                ev = jnp.exp(v - new)
                acc = ev if acc is None else acc + ev
            st_v[0, at, :] = new
            st_v[1, at, :] = acc
            for c in range(2):
                loc = ids_v[base + g:base + g + GROUP, c * LANES:(c + 1) * LANES] - me * vocab
                inside = (loc >= 0) & (loc < vocab)
                chunk = jnp.where(inside, lax.shift_right_arithmetic(loc, 7), -1)
                lane = loc & (LANES - 1)
                pick = st_v[2 + c, at, :] if t > 0 else jnp.zeros((GROUP, LANES), jnp.float32)
                for j in range(nv):
                    got = jnp.take_along_axis(xs[j], lane, axis=1, mode="promise_in_bounds")
                    pick = jnp.where(chunk == a // LANES + j, got, pick)
                st_v[2 + c, at, :] = pick

    def lm(l, t0, t1):
        rows = ROWS_LM
        for t in range(t0, t1):
            logits_of(t)
            if t > 0:
                fold(l, t - 1)
        if t1 < n_tiles:
            return
        fold(l, n_tiles - 1)
        top, total = st_v[0], st_v[1]
        peak = jnp.max(top, axis=-1, keepdims=True)
        mass = jnp.sum(total * jnp.exp(top - peak), axis=-1, keepdims=True)
        part = jnp.broadcast_to(peak + jnp.log(mass), (rows, LANES))
        tp = tails[l][0]
        for h in range(2):
            for c in range(2):
                cols = slice(c * LANES, (c + 1) * LANES)
                tp[h, 0:r2, cols] = st_v[2 + c, h * r2:(h + 1) * r2, :]
            tp[h, r2:r2 + 8, :] = part.T[0:8, :]

    r2 = ROWS_LM // 2
    tplans = []
    for l in range(len(lm_chunks)):
        tp, t1r, t2r, t3r, tc = tails[l]
        plan = {"slots": []}
        if NORTH:
            plan["pair"] = [link(tp.at[h], t1r.at[h], sibling, "quiet") for h in (0, 1)]
        else:
            plan["pair"] = [link(tp.at[1 - core], t1r.at[0], sibling)]
        for s in slots:
            a, b = coords(s)
            h = half_of[s]
            plan["slots"].append({
                "one": [link(t2r.at[s, a], t2r.at[s, a], device(s, step(a, d), b)) for d in range(1, q)],
                "two": [link(t3r.at[s, b], t3r.at[s, b], device(s, a, step(b, d))) for d in range(1, q)],
                "back": [link(tc.at[h], tc.at[h], sibling)],
            })
        tplans.append(plan)

    def join(refs, out):
        total = functools.reduce(jnp.add, [r[0:r2, :] for r in refs])
        out[0:r2, :] = total
        out[r2:r2 + 8, :] = log_add([r[r2:r2 + 8, :] for r in refs])

    def tail_pair(l):
        def go():
            for k in tplans[l]["pair"]:
                k.start()
        if NORTH:
            quiet(go)
        else:
            go()

    def tail_one(l):
        tp, t1r, t2r = tails[l][:3]

        def go():
            for k in tplans[l]["pair"]:
                k.came()
            for s in slots:
                join([tp.at[half_of[s]], t1r.at[s]], t2r.at[s, coords(s)[0]])
                for d in far_first:
                    tplans[l]["slots"][s]["one"][d - 1].start()
        talkers(go)

    def tail_two(l):
        t2r, t3r = tails[l][2:4]

        def go():
            for s in slots:
                for k in tplans[l]["slots"][s]["one"]:
                    k.came()
                join([t2r.at[s, d] for d in range(q)], t3r.at[s, coords(s)[1]])
                for d in far_first:
                    tplans[l]["slots"][s]["two"][d - 1].start()
        talkers(go)

    def tail_three(l):
        t3r, tc = tails[l][3:5]

        def go():
            for s in slots:
                for k in tplans[l]["slots"][s]["two"]:
                    k.came()
                join([t3r.at[s, d] for d in range(q)], tc.at[half_of[s]])
                for k in tplans[l]["slots"][s]["back"]:
                    k.start()
        talkers(go)

    outs = []

    def tail_done(l):
        tc = tails[l][4]

        def go():
            for s in slots:
                for k in tplans[l]["slots"][s]["back"]:
                    k.came()
        if NORTH:
            quiet(go)
        else:
            go()
        base = chunks[lm_chunks[l][0]][0]
        row = tc[0, r2:r2 + 1, :]
        lnrow_v[l:l + 1, :] = row
        lse = jnp.broadcast_to(row, (LANES, ROWS_LM)).T
        for h in range(2):
            for c in range(2):
                cols = slice(c * LANES, (c + 1) * LANES)
                ob_v[base + h * r2:base + (h + 1) * r2, cols] = (
                    tc[h, 0:r2, cols] - lse[h * r2:(h + 1) * r2, :]
                )
        i = loc_count[0]
        loc_count[0] += 1
        cp = pltpu.make_async_copy(
            ob_v.at[base:base + ROWS_LM, :], lp_hbm.at[base:base + ROWS_LM, :], loc_sems.at[i])
        cp.start()
        outs.append(cp)

    stages = [mlp, pair_send, first_send, second_send, own_block, spread_first, spread_last]
    names = {f.__name__: f for f in stages}
    names.update({f.__name__: f for f in (arrive, normalize, tail_pair, tail_one, tail_two, tail_three, tail_done)})
    for item in cfg["order"]:
        what, arg = item[0], item[1:]
        with jax.named_scope("_".join(str(v) for v in item)):
            if what == "meet":
                meet()
            elif what == "weights":
                if arg[0] < parts:
                    loads[f"w{arg[0]}"].wait()
            elif what == "ids":
                loads["ids"].wait()
            elif what == "lm":
                lm(*arg)
            else:
                names[what](*arg)

    i = loc_count[0]
    cp = pltpu.make_async_copy(lnrow_v, ln_hbm, loc_sems.at[i])
    cp.start()
    outs.append(cp)
    for cp in outs:
        cp.wait()

    def drain_talk():
        for l in started["talk"]:
            l.sent()

    talkers(drain_talk)

    def drain_quiet():
        for l in started["quiet"]:
            l.sent()

    quiet(drain_quiet)


def make_order(n_tiles):
    S1, S2, S3, S4, S5 = "first_send", "second_send", "own_block", "spread_first", "spread_last"
    order = []

    def add(*items):
        for item in items:
            order.append(item if isinstance(item, tuple) else (item,))

    add(("mlp", 0), "meet", ("pair_send", 0), ("mlp", 1), ("pair_send", 1), (S1, 0),
        ("mlp", 2), ("pair_send", 2), (S1, 1), ("mlp", 3), ("pair_send", 3), (S1, 2), "ids",
        (S2, 0), (S1, 3), (S2, 1), (S3, 0), (S2, 2), (S3, 1), (S4, 0), (S2, 3), (S3, 2), (S4, 1),
        (S3, 3), (S5, 0), (S4, 2), (S5, 1), (S4, 3), ("arrive", 0), ("arrive", 1), ("normalize", 0))
    cuts = [0, 3, 5, n_tiles]
    for i in range(3):
        for t in range(cuts[i], cuts[i + 1]):
            add(("weights", t))
        add(("lm", 0, cuts[i], cuts[i + 1]))
        if i < 2:
            add((S5, 2 + i))
    add(("tail_pair", 0), ("arrive", 2), ("arrive", 3), ("normalize", 1))
    add(("lm", 1, 0, 2), ("tail_one", 0), ("lm", 1, 2, 6), ("tail_two", 0), ("lm", 1, 6, n_tiles),
        ("tail_pair", 1), ("tail_one", 1), ("tail_three", 0), ("tail_two", 1), ("tail_done", 0),
        ("tail_three", 1), ("tail_done", 1))
    return order


def plan_chunks(batch):
    rows = ROWS_COMM
    chunks = [(i * rows, rows) for i in range(batch // rows)]
    per = ROWS_LM // rows
    return chunks, [list(range(i, i + per)) for i in range(0, len(chunks), per)]


def solution(mesh):
    n_tp = mesh.shape["tp"]
    q = math.isqrt(n_tp // CORES)

    def local_step(resid_in, cand_ids, ln_mlp, wi_gate, wi_lin, w_out, ln_final, w_lm):
        batch, width = resid_in.shape
        inner = wi_gate.shape[1]
        vocab = w_lm.shape[1]
        w_parts = -(-vocab // TILE)
        cands = cand_ids.shape[1]
        chunks, lm_chunks = plan_chunks(batch)
        n_tiles = -(-vocab // TILE)
        cfg = dict(q=q, chunks=chunks, lm=lm_chunks, w_parts=w_parts,
                   order=make_order(n_tiles))
        ns = 2 if NORTH else 1
        f32 = jnp.float32
        blocks = q * q
        bufs, tails = [], []
        for _, rows in chunks:
            r2 = rows // 2
            bufs.append((
                pltpu.VMEM((2, blocks, r2, LANES), f32),
                pltpu.VMEM((ns, blocks, r2, LANES), f32),
                pltpu.VMEM((ns, q - 1, q, r2, LANES), f32),
                pltpu.VMEM((ns, q, r2, LANES), f32),
                pltpu.VMEM((ns, q - 1, r2, LANES), f32),
                pltpu.VMEM((2, blocks, r2, LANES), f32),
            ))
        rt = ROWS_LM // 2 + 8
        for _ in lm_chunks:
            tails.append((
                pltpu.VMEM((2, rt, cands), f32),
                pltpu.VMEM((ns, rt, cands), f32),
                pltpu.VMEM((ns, q, rt, cands), f32),
                pltpu.VMEM((ns, q, rt, cands), f32),
                pltpu.VMEM((2, rt, cands), f32),
            ))
        n_links = len(chunks) * (ns * (5 * q - 3) + 2) + len(lm_chunks) * (ns * 10 + 2)
        n_loc = len(chunks) + len(lm_chunks) + w_parts + 6
        hbm = pl.BlockSpec(memory_space=pltpu.HBM)
        vmem = pl.BlockSpec(memory_space=pltpu.VMEM)
        scratch = [
            pltpu.VMEM((batch, width), jnp.bfloat16),
            pltpu.VMEM((batch, cands), jnp.int32),
            pltpu.VMEM((inner, width), jnp.bfloat16),
            pltpu.VMEM((inner, width), jnp.bfloat16),
            pltpu.VMEM((inner, width), jnp.bfloat16),
            pltpu.VMEM((vocab, width), jnp.bfloat16),
            pltpu.VMEM((ROWS_LM, width), jnp.bfloat16),
            pltpu.VMEM((2, ROWS_LM, TILE), f32),
            pltpu.VMEM((4, ROWS_LM, LANES), f32),
            pltpu.VMEM((len(lm_chunks), ROWS_LM), f32),
            pltpu.VMEM((batch, cands), f32),
            tuple(bufs),
            tuple(tails),
            pltpu.SemaphoreType.DMA((n_links,)),
            pltpu.SemaphoreType.DMA((n_links,)),
            pltpu.SemaphoreType.DMA((n_loc,)),
        ]
        log_probs, log_norm = pl.pallas_call(
            functools.partial(fused, cfg),
            out_shape=(
                jax.ShapeDtypeStruct((batch, cands), f32),
                jax.ShapeDtypeStruct((len(lm_chunks), ROWS_LM), f32),
            ),
            in_specs=[hbm, hbm, vmem, hbm, hbm, hbm, vmem, hbm],
            out_specs=(hbm, hbm),
            scratch_shapes=scratch,
            compiler_params=pltpu.CompilerParams(
                collective_id=0, has_side_effects=True, vmem_limit_bytes=67_043_328),
            name="fused",
        )(resid_in, cand_ids, ln_mlp, wi_gate.T, wi_lin.T, w_out, ln_final, w_lm.T)
        return log_probs, log_norm.reshape(batch)

    in_specs = (P("dp", None), P("dp", None), P(None), P(None, "tp"), P(None, "tp"), P("tp", None), P(None), P(None, "tp"))
    return jax.shard_map(local_step, mesh=mesh, in_specs=in_specs, out_specs=(P("dp", None), P("dp")), check_vma=False)
```

```python
import functools
import math

import jax
import jax.numpy as jnp
from jax import lax
from jax.experimental import pallas as pl
from jax.experimental.pallas import tpu as pltpu
from jax.sharding import PartitionSpec as P

EPS = 1e-6
LANES = 128
CORES = 2
MESH = pl.DeviceIdType.MESH
NEG = float("-inf")

NORTH = False
ROWS_LM = 128
ROWS_COMM = 128
TILE = 256
PIECE = 256
RING = 4
TRANS_B = (((1,), (1,)), ((), ()))


def rms_rows(wide, scale):
    mean_sq = jnp.mean(wide * wide, axis=-1, keepdims=True)
    return (wide * lax.rsqrt(mean_sq + EPS) * scale).astype(jnp.bfloat16)


def log_add(parts):
    top = functools.reduce(jnp.maximum, parts)
    total = functools.reduce(jnp.add, [jnp.exp(p - top) for p in parts])
    return top + jnp.log(total)


class Link:
    def __init__(self, src, dst, send, recv, to):
        self.args = dict(
            src_ref=src, dst_ref=dst, send_sem=send, recv_sem=recv,
            device_id={"tp": to}, device_id_type=MESH,
        )

    def make(self):
        return pltpu.make_async_remote_copy(**self.args)

    def start(self):
        self.make().start()

    def sent(self):
        self.make().wait_send()

    def came(self):
        self.make().wait_recv()


def fused(cfg, x_hbm, ids_hbm, lnm_ref, wg_hbm, wl_hbm, wo_hbm, lnf_ref, w_hbm,
          lp_hbm, ln_hbm,
          x_v, ids_v, wg_v, wl_v, wo_v, w_v, wr_v, we_v, z_v, lg_v, st_v, id_v, lnrow_v, ob_v,
          bufs, tails, send_sems, recv_sems, loc_sems, w_sems, free_sem):
    q, chunks, lm_chunks = cfg["q"], cfg["chunks"], cfg["lm"]
    me = lax.axis_index("tp")
    core = lax.rem(me, CORES)
    x = lax.rem(me // CORES, q)
    y = me // (CORES * q)
    sibling = me + 1 - 2 * core
    vocab = w_hbm.shape[0]
    padded = w_v.shape[1]
    pieces = vocab // PIECE
    rest = vocab - pieces * PIECE
    ndev_side = q

    if NORTH:
        slots = [0, 1]
        half_of = [0, 1]
        speak = 1
    else:
        slots = [0]
        half_of = [core]
        speak = core

    def coords(s):
        if NORTH:
            return (x, y) if s == 0 else (y, x)
        a = jnp.where(core == 0, x, y)
        b = jnp.where(core == 0, y, x)
        return a, b

    def device(s, a, b):
        if NORTH:
            col, row = (a, b) if s == 0 else (b, a)
            return (row * q + col) * CORES + 1
        col = jnp.where(core == 0, a, b)
        row = jnp.where(core == 0, b, a)
        return (row * q + col) * CORES + core

    def step(v, d):
        return lax.rem(v + d + q, q)

    far_first = sorted(range(1, q), key=lambda d: -min(d, q - d))

    counter = [0]
    started = {"all": [], "talk": [], "quiet": []}

    def link(src, dst, to, who="talk"):
        i = counter[0]
        counter[0] += 1
        made = Link(src, dst, send_sems.at[i], recv_sems.at[i], to)
        started[who].append(made)
        return made

    def talkers(fn):
        if NORTH:
            pl.when(core == 1)(fn)
        else:
            fn()

    def quiet(fn):
        if NORTH:
            pl.when(core == 0)(fn)

    loads = {}
    loc_count = [0]

    def load(name, src, dst):
        i = loc_count[0]
        loc_count[0] += 1
        cp = pltpu.make_async_copy(src, dst, loc_sems.at[i])
        loads[name] = cp
        cp.start()

    off0, rows0 = chunks[0]
    load("x0", x_hbm.at[pl.ds(off0, rows0), :], x_v.at[pl.ds(off0, rows0), :])
    load("wg", wg_hbm, wg_v)
    load("wl", wl_hbm, wl_v)
    load("wo", wo_hbm, wo_v)
    for k, (off, rows) in enumerate(chunks[1:], 1):
        load(f"x{k}", x_hbm.at[pl.ds(off, rows), :], x_v.at[pl.ds(off, rows), :])
    load("ids", ids_hbm, ids_v)
    def piece(p):
        return pltpu.make_async_copy(
            w_hbm.at[pl.ds(pl.multiple_of(p * PIECE, PIECE), PIECE), :],
            wr_v.at[lax.rem(p, RING)], w_sems.at[lax.rem(p, RING)])

    for p in range(min(RING, pieces)):
        piece(jnp.int32(p)).start()
    load("rest", w_hbm.at[pl.ds(pieces * PIECE, rest), :], we_v)

    def turn(p0, p1):
        def one(p, carry):
            piece(p).wait()
            slot = lax.rem(p, RING)
            cols = pl.ds(pl.multiple_of(p * PIECE, PIECE), PIECE)
            for j in range(q * q):
                band = slice(j * LANES, (j + 1) * LANES)
                w_v[band, cols] = wr_v[slot, :, band].T
            pl.when(p + RING < pieces)(lambda: piece(p + RING).start())
            return carry

        lax.fori_loop(p0, min(p1, pieces), one, 0)
        if p1 > pieces:
            loads["rest"].wait()
            for j in range(q * q):
                band = slice(j * LANES, (j + 1) * LANES)
                w_v[band, pieces * PIECE:vocab] = we_v[:, band].T

    barrier = pltpu.get_barrier_semaphore()

    def greet(to):
        pl.semaphore_signal(barrier, inc=1, device_id={"tp": to}, device_id_type=MESH)

    greet(sibling)

    def greet_far():
        a, b = coords(0)
        for d in range(1, q):
            greet(device(0, step(a, d), b))
            greet(device(0, a, step(b, d)))

    talkers(greet_far)

    def meet():
        if NORTH:
            pl.when(core == 1)(lambda: pl.semaphore_wait(barrier, 1 + 2 * (q - 1)))
            pl.when(core == 0)(lambda: pl.semaphore_wait(barrier, 1))
        else:
            pl.semaphore_wait(barrier, 1 + 2 * (q - 1))

    scale_mlp = lnm_ref[...].astype(jnp.float32).reshape(1, -1)
    scale_fin = lnf_ref[...].astype(jnp.float32).reshape(1, -1)

    plans = []
    for k, (off, rows) in enumerate(chunks):
        r2 = rows // 2
        px, dr, rl, bs, pr = bufs[k]
        xb = px
        plan = {"slots": []}
        if NORTH:
            plan["pair"] = [link(px.at[h], dr.at[h], sibling, "quiet") for h in (0, 1)]
        else:
            plan["pair"] = [link(px.at[1 - core], dr.at[0], sibling)]
        for s in slots:
            a, b = coords(s)
            h = half_of[s]

            def grp(v):
                return pl.ds(v * q, q)

            e = {}
            e["one"] = [
                link(dr.at[s, grp(step(a, d))], rl.at[s, d - 1], device(s, step(a, d), b))
                for d in range(1, q)
            ]
            e["second"] = [
                link(bs.at[s, step(b, d)], pr.at[s, d - 1], device(s, a, step(b, d)))
                for d in range(1, q)
            ]
            own = xb.at[h, a * q + b]
            e["spread2"] = [link(own, own, device(s, a, step(b, d))) for d in range(1, q)]
            mine = xb.at[h, grp(a)]
            e["wide"] = [link(mine, mine, device(s, step(a, d), b)) for d in range(1, q)]
            e["pass"] = [
                link(xb.at[h, grp(step(a, d))], xb.at[h, grp(step(a, d))], sibling)
                for d in range(q)
            ]
            plan["slots"].append(e)
        plans.append(plan)

    def mlp(k):
        off, rows = chunks[k]
        px = bufs[k][0]
        r2 = rows // 2
        loads[f"x{k}"].wait()
        wide = x_v[pl.ds(off, rows), :].astype(jnp.float32)
        normed = rms_rows(wide, scale_mlp)
        if k == 0:
            loads["wg"].wait()
            loads["wl"].wait()
        gate = lax.dot_general(normed, wg_v[...], TRANS_B, preferred_element_type=jnp.float32)
        lin = lax.dot_general(normed, wl_v[...], TRANS_B, preferred_element_type=jnp.float32)
        hidden = (jax.nn.gelu(gate, approximate=True) * lin).astype(jnp.bfloat16)
        if k == 0:
            loads["wo"].wait()
        part = jnp.dot(hidden, wo_v[...], preferred_element_type=jnp.float32)
        for h in range(2):
            for j in range(q * q):
                px[h, j] = part[h * r2:(h + 1) * r2, j * LANES:(j + 1) * LANES]

    def pair_send(k):
        def go():
            for l in plans[k]["pair"]:
                l.start()
        if NORTH:
            quiet(go)
        else:
            go()

    def first_send(k):
        px, dr = bufs[k][0], bufs[k][1]

        def go():
            for l in plans[k]["pair"]:
                l.came()
                l.sent()
            pl.semaphore_signal(free_sem, inc=1, device_id={"tp": sibling}, device_id_type=MESH)
            for s in slots:
                a, _ = coords(s)
                h = half_of[s]
                e = plans[k]["slots"][s]
                for d in far_first + [0]:
                    g = pl.ds(step(a, d) * q, q)
                    dr[s, g] = dr[s, g] + px[h, g]
                    if d:
                        e["one"][d - 1].start()
        talkers(go)

    def second_send(k):
        _, dr, rl, bs = bufs[k][:4]

        def go():
            for s in slots:
                a, _ = coords(s)
                e = plans[k]["slots"][s]
                for l in e["one"]:
                    l.came()
                total = dr[s, pl.ds(a * q, q)]
                for d in range(q - 1):
                    total = total + rl[s, d]
                bs[s] = total
                for d in far_first:
                    e["second"][d - 1].start()
        talkers(go)

    def own_block(k):
        off, rows = chunks[k]
        r2 = rows // 2
        xb, _, _, bs, pr = bufs[k]

        def go():
            for s in slots:
                a, b = coords(s)
                h = half_of[s]
                e = plans[k]["slots"][s]
                for l in e["second"]:
                    l.came()
                total = bs[s, b]
                for d in range(q - 1):
                    total = total + pr[s, d]
                col = pl.ds(pl.multiple_of((a * q + b) * LANES, LANES), LANES)
                row = pl.ds(pl.multiple_of(off + h * r2, 16), r2)
                resid = x_v[row, col].astype(jnp.float32)
                xb[h, a * q + b] = (resid + total).astype(jnp.bfloat16).astype(jnp.float32)
                for d in far_first:
                    e["spread2"][d - 1].start()
        talkers(go)

    def spread_first(k):
        def go():
            for s in slots:
                e = plans[k]["slots"][s]
                for l in e["spread2"]:
                    l.came()
                for d in far_first:
                    e["wide"][d - 1].start()
                pl.semaphore_wait(free_sem, 1)
                e["pass"][0].start()
        talkers(go)

    def spread_last(k):
        def go():
            for s in slots:
                e = plans[k]["slots"][s]
                for d in reversed(far_first):
                    e["wide"][d - 1].came()
                    e["pass"][q - d].start()
        talkers(go)

    def arrive(k):
        def go():
            for s in slots:
                for l in plans[k]["slots"][s]["pass"]:
                    l.came()
        if NORTH:
            quiet(go)
        else:
            go()

    def normalize(l):
        first = lm_chunks[l]
        base = chunks[first[0]][0]
        for c in range(2):
            loc = ids_v[base:base + ROWS_LM, c * LANES:(c + 1) * LANES] - me * vocab
            inside = (loc >= 0) & (loc < vocab)
            id_v[c] = loc & (LANES - 1)
            id_v[2 + c] = jnp.where(inside, lax.shift_right_arithmetic(loc, 7), -1)
        for k in first:
            off, rows = chunks[k]
            r2 = rows // 2
            xb = bufs[k][0]
            for h in range(2):
                sq = None
                for j in range(q * q):
                    v = xb[h, j]
                    sq = v * v if sq is None else sq + v * v
                mean_sq = jnp.sum(sq, axis=-1, keepdims=True) * (1.0 / (q * q * LANES))
                inv = jnp.broadcast_to(lax.rsqrt(mean_sq + EPS), (r2, LANES))
                for j in range(q * q):
                    cols = slice(j * LANES, (j + 1) * LANES)
                    z_v[off - base + h * r2:off - base + (h + 1) * r2, cols] = (
                        xb[h, j] * inv * scale_fin[:, cols]
                    ).astype(jnp.bfloat16)

    n_tiles = -(-vocab // TILE)

    ids = [None] * 4

    def logits_of(t):
        a = t * TILE
        wd = min(TILE, padded - a)
        lg_v[t % 2, :, :wd] = jnp.dot(z_v[...], w_v[:, a:a + wd], preferred_element_type=jnp.float32)

    def fold(t, state):
        a = t * TILE
        wd = min(TILE, vocab - a)
        nv = -(-wd // LANES)
        xs = [lg_v[t % 2, :, j * LANES:(j + 1) * LANES] for j in range(nv)]
        if wd % LANES:
            pos = lax.broadcasted_iota(jnp.int32, (ROWS_LM, LANES), 1)
            xs[-1] = jnp.where(pos < wd % LANES, xs[-1], NEG)
        new = functools.reduce(jnp.maximum, xs)
        acc = None
        if t > 0:
            new = jnp.maximum(state[0], new)
            acc = state[1] * jnp.exp(state[0] - new)
        for v in xs:
            ev = jnp.exp(v - new)
            acc = ev if acc is None else acc + ev
        picks = []
        for c in range(2):
            pick = state[2 + c] if t > 0 else jnp.zeros((ROWS_LM, LANES), jnp.float32)
            for j in range(nv):
                got = jnp.take_along_axis(xs[j], ids[c], axis=1, mode="promise_in_bounds")
                pick = jnp.where(ids[2 + c] == a // LANES + j, got, pick)
            picks.append(pick)
        return [new, acc] + picks

    def lm(l, t0, t1):
        rows = ROWS_LM
        ids[:] = [id_v[i] for i in range(4)]
        state = [st_v[i] for i in range(4)] if t0 > 1 else None
        for t in range(t0, t1):
            if t > 0:
                state = fold(t - 1, state)
            logits_of(t)
        if t1 < n_tiles:
            for i in range(4):
                st_v[i] = state[i]
            return
        state = fold(n_tiles - 1, state)
        for i in range(4):
            st_v[i] = state[i]
        top, total = st_v[0], st_v[1]
        peak = jnp.max(top, axis=-1, keepdims=True)
        mass = jnp.sum(total * jnp.exp(top - peak), axis=-1, keepdims=True)
        part = jnp.broadcast_to(peak + jnp.log(mass), (rows, LANES))
        tp = tails[l][0]
        for h in range(2):
            for c in range(2):
                cols = slice(c * LANES, (c + 1) * LANES)
                tp[h, 0:r2, cols] = st_v[2 + c, h * r2:(h + 1) * r2, :]
                tp[h, r2:r2 + 8, cols] = part.T[0:8, :]

    r2 = ROWS_LM // 2
    tplans = []
    for l in range(len(lm_chunks)):
        tp, t1r, t2r, t3r, tc = tails[l]
        plan = {"slots": []}
        if NORTH:
            plan["pair"] = [link(tp.at[h], t1r.at[h], sibling, "quiet") for h in (0, 1)]
        else:
            plan["pair"] = [link(tp.at[1 - core], t1r.at[0], sibling)]
        for s in slots:
            a, b = coords(s)
            h = half_of[s]
            plan["slots"].append({
                "one": [link(t2r.at[s, a], t2r.at[s, a], device(s, step(a, d), b)) for d in range(1, q)],
                "two": [link(t3r.at[s, b], t3r.at[s, b], device(s, a, step(b, d))) for d in range(1, q)],
                "back": [link(tc.at[h], tc.at[h], sibling)],
            })
        tplans.append(plan)

    def join(refs, out):
        total = functools.reduce(jnp.add, [r[0:r2, :] for r in refs])
        out[0:r2, :] = total
        out[r2:r2 + 8, :] = log_add([r[r2:r2 + 8, :] for r in refs])

    def tail_pair(l):
        def go():
            for k in tplans[l]["pair"]:
                k.start()
        if NORTH:
            quiet(go)
        else:
            go()

    def tail_one(l):
        tp, t1r, t2r = tails[l][:3]

        def go():
            for k in tplans[l]["pair"]:
                k.came()
            for s in slots:
                join([tp.at[half_of[s]], t1r.at[s]], t2r.at[s, coords(s)[0]])
                for d in far_first:
                    tplans[l]["slots"][s]["one"][d - 1].start()
        talkers(go)

    def tail_two(l):
        t2r, t3r = tails[l][2:4]

        def go():
            for s in slots:
                for k in tplans[l]["slots"][s]["one"]:
                    k.came()
                join([t2r.at[s, d] for d in range(q)], t3r.at[s, coords(s)[1]])
                for d in far_first:
                    tplans[l]["slots"][s]["two"][d - 1].start()
        talkers(go)

    def tail_three(l):
        t3r, tc = tails[l][3:5]

        def go():
            for s in slots:
                for k in tplans[l]["slots"][s]["two"]:
                    k.came()
                join([t3r.at[s, d] for d in range(q)], tc.at[half_of[s]])
                for k in tplans[l]["slots"][s]["back"]:
                    k.start()
        talkers(go)

    outs = []

    def tail_done(l):
        tc = tails[l][4]

        def go():
            for s in slots:
                for k in tplans[l]["slots"][s]["back"]:
                    k.came()
        if NORTH:
            quiet(go)
        else:
            go()
        base = chunks[lm_chunks[l][0]][0]
        row = tc[0, r2:r2 + 1, 0:ROWS_LM]
        lnrow_v[l:l + 1, :] = row
        lse = jnp.broadcast_to(row, (LANES, ROWS_LM)).T
        for h in range(2):
            for c in range(2):
                cols = slice(c * LANES, (c + 1) * LANES)
                ob_v[base + h * r2:base + (h + 1) * r2, cols] = (
                    tc[h, 0:r2, cols] - lse[h * r2:(h + 1) * r2, :]
                )
        i = loc_count[0]
        loc_count[0] += 1
        cp = pltpu.make_async_copy(
            ob_v.at[base:base + ROWS_LM, :], lp_hbm.at[base:base + ROWS_LM, :], loc_sems.at[i])
        cp.start()
        outs.append(cp)

    stages = [mlp, pair_send, first_send, second_send, own_block, spread_first, spread_last]
    names = {f.__name__: f for f in stages}
    names.update({f.__name__: f for f in (turn, arrive, normalize, tail_pair, tail_one, tail_two, tail_three, tail_done)})
    for item in cfg["order"]:
        what, arg = item[0], item[1:]
        with jax.named_scope("_".join(str(v) for v in item)):
            if what == "meet":
                meet()
            elif what == "weights":
                pass
            elif what == "ids":
                loads["ids"].wait()
            elif what == "lm":
                lm(*arg)
            else:
                names[what](*arg)

    i = loc_count[0]
    cp = pltpu.make_async_copy(lnrow_v, ln_hbm, loc_sems.at[i])
    cp.start()
    outs.append(cp)
    for cp in outs:
        cp.wait()

    def drain_talk():
        early = [l for p in plans for l in p["pair"]]
        for l in started["talk"]:
            if l not in early:
                l.sent()

    talkers(drain_talk)

    def drain_quiet():
        for l in started["quiet"]:
            l.sent()

    quiet(drain_quiet)


def make_order(n_tiles, n_turns):
    S1, S2, S3, S4, S5 = "first_send", "second_send", "own_block", "spread_first", "spread_last"
    order = []
    turned = [0]
    cut = n_tiles * 5 // 8

    def add(*items):
        for item in items:
            order.append(item if isinstance(item, tuple) else (item,))

    def turn(count):
        upto = min(n_turns, turned[0] + count)
        if upto > turned[0]:
            add(("turn", turned[0], upto))
        turned[0] = upto

    def whole(l):
        add(("arrive", l), ("normalize", l), ("lm", l, 0, n_tiles), ("tail_pair", l))

    add(("mlp", 0), "meet", ("pair_send", 0), ("mlp", 1), ("pair_send", 1), (S1, 0),
        ("mlp", 2), ("pair_send", 2), (S1, 1), ("mlp", 3), ("pair_send", 3), (S1, 2), "ids")
    turn(11)
    add((S2, 0), (S1, 3))
    turn(6)
    add((S2, 1))
    turn(5)
    add((S3, 0))
    turn(4)
    add((S2, 2), (S3, 1))
    turn(3)
    add((S4, 0), (S2, 3))
    turn(n_turns)
    add((S3, 2), (S4, 1), (S3, 3), (S5, 0), (S4, 2))
    whole(0)
    add((S5, 1), (S4, 3))
    whole(1)
    add((S5, 2), ("tail_one", 0))
    whole(2)
    add((S5, 3), ("tail_one", 1), ("tail_two", 0))
    add(("arrive", 3), ("normalize", 3), ("lm", 3, 0, cut),
        ("tail_one", 2), ("tail_two", 1), ("tail_three", 0), ("lm", 3, cut, n_tiles), ("tail_pair", 3),
        ("tail_done", 0), ("tail_one", 3), ("tail_two", 2), ("tail_three", 1), ("tail_two", 3),
        ("tail_done", 1), ("tail_three", 2), ("tail_three", 3), ("tail_done", 2), ("tail_done", 3))
    return order


def plan_chunks(batch):
    rows = ROWS_COMM
    chunks = [(i * rows, rows) for i in range(batch // rows)]
    per = ROWS_LM // rows
    return chunks, [list(range(i, i + per)) for i in range(0, len(chunks), per)]


def solution(mesh):
    n_tp = mesh.shape["tp"]
    q = math.isqrt(n_tp // CORES)

    def local_step(resid_in, cand_ids, ln_mlp, wi_gate, wi_lin, w_out, ln_final, w_lm):
        batch, width = resid_in.shape
        inner = wi_gate.shape[1]
        vocab = w_lm.shape[1]
        whole = vocab // PIECE
        padded = -(-vocab // LANES) * LANES
        cands = cand_ids.shape[1]
        chunks, lm_chunks = plan_chunks(batch)
        n_tiles = -(-vocab // TILE)
        cfg = dict(q=q, chunks=chunks, lm=lm_chunks,
                   order=make_order(n_tiles, whole + 1))
        ns = 2 if NORTH else 1
        f32 = jnp.float32
        blocks = q * q
        bufs, tails = [], []
        for _, rows in chunks:
            r2 = rows // 2
            bufs.append((
                pltpu.VMEM((2, blocks, r2, LANES), f32),
                pltpu.VMEM((ns, blocks, r2, LANES), f32),
                pltpu.VMEM((ns, q - 1, q, r2, LANES), f32),
                pltpu.VMEM((ns, q, r2, LANES), f32),
                pltpu.VMEM((ns, q - 1, r2, LANES), f32),
            ))
        rt = ROWS_LM // 2 + 8
        for _ in lm_chunks:
            tails.append((
                pltpu.VMEM((2, rt, cands), f32),
                pltpu.VMEM((ns, rt, cands), f32),
                pltpu.VMEM((ns, q, rt, cands), f32),
                pltpu.VMEM((ns, q, rt, cands), f32),
                pltpu.VMEM((2, rt, cands), f32),
            ))
        n_links = len(chunks) * (ns * (5 * q - 3) + 2) + len(lm_chunks) * (ns * 10 + 2)
        n_loc = len(chunks) + len(lm_chunks) + 8
        hbm = pl.BlockSpec(memory_space=pltpu.HBM)
        vmem = pl.BlockSpec(memory_space=pltpu.VMEM)
        scratch = [
            pltpu.VMEM((batch, width), jnp.bfloat16),
            pltpu.VMEM((batch, cands), jnp.int32),
            pltpu.VMEM((inner, width), jnp.bfloat16),
            pltpu.VMEM((inner, width), jnp.bfloat16),
            pltpu.VMEM((inner, width), jnp.bfloat16),
            pltpu.VMEM((width, padded), jnp.bfloat16),
            pltpu.VMEM((RING, PIECE, width), jnp.bfloat16),
            pltpu.VMEM((vocab - whole * PIECE, width), jnp.bfloat16),
            pltpu.VMEM((ROWS_LM, width), jnp.bfloat16),
            pltpu.VMEM((2, ROWS_LM, TILE), f32),
            pltpu.VMEM((4, ROWS_LM, LANES), f32),
            pltpu.VMEM((4, ROWS_LM, LANES), jnp.int32),
            pltpu.VMEM((len(lm_chunks), ROWS_LM), f32),
            pltpu.VMEM((batch, cands), f32),
            tuple(bufs),
            tuple(tails),
            pltpu.SemaphoreType.DMA((n_links,)),
            pltpu.SemaphoreType.DMA((n_links,)),
            pltpu.SemaphoreType.DMA((n_loc,)),
            pltpu.SemaphoreType.DMA((RING,)),
            pltpu.SemaphoreType.REGULAR,
        ]
        log_probs, log_norm = pl.pallas_call(
            functools.partial(fused, cfg),
            out_shape=(
                jax.ShapeDtypeStruct((batch, cands), f32),
                jax.ShapeDtypeStruct((len(lm_chunks), ROWS_LM), f32),
            ),
            in_specs=[hbm, hbm, vmem, hbm, hbm, hbm, vmem, hbm],
            out_specs=(hbm, hbm),
            scratch_shapes=scratch,
            compiler_params=pltpu.CompilerParams(
                collective_id=0, has_side_effects=True, vmem_limit_bytes=67_043_328),
            name="fused",
        )(resid_in, cand_ids, ln_mlp, wi_gate.T, wi_lin.T, w_out, ln_final, w_lm.T)
        return log_probs, log_norm.reshape(batch)

    in_specs = (P("dp", None), P("dp", None), P(None), P(None, "tp"), P(None, "tp"), P("tp", None), P(None), P(None, "tp"))
    return jax.shard_map(local_step, mesh=mesh, in_specs=in_specs, out_specs=(P("dp", None), P("dp")), check_vma=False)
```
